256 devices in a mesh: gx: 8 (over y, z_lo), gy: 4 (over z_hi), gz: 8 (over x, core).
Axes of the slice: x: 4, y: 4, z: 8 (z_hi: 4, z_lo: 2; z = z_hi * 2 + z_lo), core: 2. Of those that a mesh axis runs over, the one named last changes fastest.
Arguments:
- node_latent: bfloat16 [8, 4, 8, 512, 128], P('gx', 'gy', 'gz'), may hold values from -6 to 6
- ghost_latent: bfloat16 [8, 4, 8, 6, 64, 128], P('gx', 'gy', 'gz'), may hold values from -6 to 6
- edge_latent: bfloat16 [8, 4, 8, 2816, 128], P('gx', 'gy', 'gz'), may hold values from -6 to 6
- senders: int32 [8, 4, 8, 2816], P('gx', 'gy', 'gz'), may hold values from 0 to 895
- receivers: int32 [8, 4, 8, 2816], P('gx', 'gy', 'gz'), may hold values from 0 to 511, never falling along the last dimension, each value on 1 to 12 neighbouring positions
- export_rows: int32 [8, 4, 8, 6, 64], P('gx', 'gy', 'gz'), may hold values from 0 to 512, as said below
- node_cotangent: bfloat16 [8, 4, 8, 512, 128], P('gx', 'gy', 'gz'), may hold values from -6 to 6
- edge_cotangent: bfloat16 [8, 4, 8, 2816, 128], P('gx', 'gy', 'gz'), may hold values from -6 to 6
- w_edge_in: bfloat16 [384, 128], replicated, may hold values from -0.3125 to 0.3125
- w_edge_hidden: bfloat16 [2, 128, 128], replicated, may hold values from -0.5 to 0.5
- b_edge: float32 [3, 128], replicated, may hold values from -3 to 3
- gain_edge: float32 [128], replicated, may hold values from 0.1 to 1.9
- shift_edge: float32 [128], replicated, may hold values from -3 to 3
- w_node_in: bfloat16 [256, 128], replicated, may hold values from -0.375 to 0.375
- w_node_hidden: bfloat16 [2, 128, 128], replicated, may hold values from -0.5 to 0.5
- b_node: float32 [3, 128], replicated, may hold values from -3 to 3
- gain_node: float32 [128], replicated, may hold values from 0.1 to 1.9
Outputs:
- node_grad: float32 [8, 4, 8, 512, 128], P('gx', 'gy', 'gz')
- edge_grad: bfloat16 [8, 4, 8, 2816, 128], P('gx', 'gy', 'gz')
- grad_w_edge_in: float32 [384, 128], replicated
- grad_w_edge_hidden: float32 [2, 128, 128], replicated
- grad_b_edge: float32 [3, 128], replicated
- grad_gain_edge: float32 [128], replicated
- grad_shift_edge: float32 [128], replicated
- grad_w_node_in: float32 [256, 128], replicated
- grad_w_node_hidden: float32 [2, 128, 128], replicated
- grad_b_node: float32 [3, 128], replicated
- grad_gain_node: float32 [128], replicated
The draws below stay inside these ranges and needn't reach their ends.
Inputs may be any that keep to these rules, and one draw needn't show every extreme that they name: `export_rows`: for each block and face the leading slots hold distinct owned rows of that block; the remaining slots hold 512, marking an empty slot.
All inputs are finite; a program needn't handle non-finite values.
Results may differ from the reference program's by a relative error of at most 0.02.
Values sent between devices are 32-bit elements; how exact they have to be, the bound alone decides.
A program may use at most 64 MiB of HBM per device.

```python
import math
import jax
import jax.numpy as jnp
import numpy as np
from jax import lax

D = 128
NODES_PER_BLOCK = 512
GHOST_SLOTS = 64
EDGE_DEV = 2816
NODES = 131072
EDGES = 720896
N_GX = 8
N_GY = 4
N_GZ = 8


def draw_export_rows(key, part):
    slab_count = N_GX * N_GY * N_GZ * 6
    slab_keys = jax.random.split(jax.random.fold_in(key, 11), slab_count)

    def one_slab(slab_key):
        order_key, vacant_random_key = jax.random.split(slab_key)
        picked_slots = jax.random.permutation(order_key, NODES_PER_BLOCK)[:GHOST_SLOTS].astype(jnp.int32)
        vacant_slots = jax.random.randint(vacant_random_key, (), 0, GHOST_SLOTS // 4 + 1, dtype=jnp.int32)
        ghost_positions = jnp.arange(GHOST_SLOTS, dtype=jnp.int32)
        return jnp.where(ghost_positions < GHOST_SLOTS - vacant_slots, picked_slots, NODES_PER_BLOCK).astype(jnp.int32)
    return jax.vmap(one_slab)(slab_keys).reshape(N_GX, N_GY, N_GZ, 6, GHOST_SLOTS)


def set_ends(values, rng, low, top_value):
    longest = values.shape.index(max(values.shape))
    spots = []
    for shift in (0, 1):
        where = [jax.random.randint(jax.random.fold_in(rng, axis), (), 0, length) for axis, length in enumerate(values.shape)]
        where[longest] = (where[longest] + shift) % values.shape[longest]
        spots.append(tuple(where))
    return values.at[spots[0]].set(low).at[spots[1]].set(top_value)


def shard_levels(own_key, extent, cuts, low, largest):
    level = 1.0
    for dim, shards_of in cuts:
        draws = jax.random.uniform(jax.random.fold_in(jax.random.fold_in(own_key, 6), dim), (shards_of,), jnp.float32, low / len(cuts), largest / len(cuts))
        level = level * jnp.repeat(jnp.exp(draws), extent[dim] // shards_of).reshape((-1,) + (1,) * (len(extent) - 1 - dim))
    return level


def split_up(amount, total, limit, slope):
    portions = [(1 << 20) // math.isqrt(standing ** slope) + 1 for standing in range(2, amount + 1)]
    rest, counts = total - limit - (amount - 1), [1] * (amount - 1)
    while rest > 0:
        free = [i for i in range(amount - 1) if counts[i] < limit]
        whole, remaining = sum([portions[i] for i in free]), rest
        for i in free:
            addition = min(limit - counts[i], max(1, remaining * portions[i] // whole), rest)
            counts[i] = counts[i] + addition
            rest = rest - addition
    return np.array([limit] + counts)


def uneven_parts(stream_key, count, total, most, skew):
    if count == 2:
        one = jax.random.randint(stream_key, (), max(1, total - most), min(most, total - 1) + 1)
        return jnp.stack([one, total - one])
    lengths = jnp.asarray(split_up(count, total, most, skew), jnp.int32)
    pairs = (count - 1) // 2
    source_of, receiver = lengths[1:1 + 2 * pairs:2], lengths[2:2 + 2 * pairs:2]
    slack = jnp.minimum(source_of - 1, most - receiver)
    passed = jax.random.randint(jax.random.fold_in(stream_key, 1), (pairs,), 0, 1 << 20) % (slack + 1)
    lengths = lengths.at[1:1 + 2 * pairs:2].set(source_of - passed).at[2:2 + 2 * pairs:2].set(receiver + passed)
    return lengths[jax.random.permutation(jax.random.fold_in(stream_key, 2), count)]


def gaussian(key, dims, scale, bound, cuts=(), kind=jnp.bfloat16):
    result = jax.random.normal(key, dims, jnp.float32) * scale
    if len(cuts) > 0:
        result = shard_levels(key, dims, cuts, -0.22, 0.18) * result
    return jnp.clip(result, min=-bound, max=bound).astype(kind)


def setup_inputs(seed: int = 0) -> dict:
    key_of = jax.random.split(jax.random.key(seed), 18)
    node_latent = gaussian(key_of[0], (N_GX, N_GY, N_GZ, NODES_PER_BLOCK, D), 1.0, 6.0, ((0, 8), (1, 4), (2, 8)))
    ghost_latent = gaussian(key_of[1], (N_GX, N_GY, N_GZ, 6, GHOST_SLOTS, D), 1.0, 6.0, ((0, 8), (1, 4), (2, 8)))
    edge_latent = gaussian(key_of[2], (N_GX, N_GY, N_GZ, EDGE_DEV, D), 1.0, 6.0, ((0, 8), (1, 4), (2, 8)))
    senders = set_ends(jax.random.randint(key_of[3], (N_GX, N_GY, N_GZ, EDGE_DEV), 0, NODES_PER_BLOCK + 6 * GHOST_SLOTS), jax.random.fold_in(key_of[3], 1), 0, (NODES_PER_BLOCK + 6 * GHOST_SLOTS) - 1).astype(jnp.int32)
    receivers = jax.vmap(lambda own: jnp.searchsorted(jnp.cumsum(uneven_parts(own, NODES_PER_BLOCK, EDGE_DEV, 12, 1)), jnp.arange(EDGE_DEV), side="right"))(jax.random.split(key_of[4], N_GX * N_GY * N_GZ)).reshape((N_GX, N_GY, N_GZ, EDGE_DEV)).astype(jnp.int32)
    export_rows = draw_export_rows(jax.random.fold_in(key_of[17], 71), 0)
    node_cotangent = gaussian(key_of[6], (N_GX, N_GY, N_GZ, NODES_PER_BLOCK, D), 1.0, 6.0, ((0, 8), (1, 4), (2, 8)))
    edge_cotangent = gaussian(key_of[7], (N_GX, N_GY, N_GZ, EDGE_DEV, D), 1.0, 6.0, ((0, 8), (1, 4), (2, 8)))
    w_edge_in = gaussian(key_of[8], (3 * D, D), (3 * D) ** -0.5, 0.3125)
    w_edge_hidden = gaussian(key_of[9], (2, D, D), D ** -0.5, 0.5)
    b_edge = gaussian(key_of[10], (3, D), 0.5, 3.0, (), jnp.float32)
    gain_edge = jnp.clip(1.0 + 0.18 * jax.random.normal(key_of[11], (D,), jnp.float32), 0.1, 1.9)
    shift_edge = gaussian(key_of[12], (D,), 0.5, 3.0, (), jnp.float32)
    w_node_in = gaussian(key_of[13], (2 * D, D), (2 * D) ** -0.5, 0.375)
    w_node_hidden = gaussian(key_of[14], (2, D, D), D ** -0.5, 0.5)
    b_node = gaussian(key_of[15], (3, D), 0.5, 3.0, (), jnp.float32)
    gain_node = jnp.clip(1.0 + 0.18 * jax.random.normal(key_of[16], (D,), jnp.float32), 0.1, 1.9)
    return dict(node_latent=node_latent, ghost_latent=ghost_latent, edge_latent=edge_latent, senders=senders, receivers=receivers, export_rows=export_rows, node_cotangent=node_cotangent, edge_cotangent=edge_cotangent, w_edge_in=w_edge_in, w_edge_hidden=w_edge_hidden, b_edge=b_edge, gain_edge=gain_edge, shift_edge=shift_edge, w_node_in=w_node_in, w_node_hidden=w_node_hidden, b_node=b_node, gain_node=gain_node)


EPSILON = 1e-05

def matmul(left, right):
    return jnp.dot(left, right, preferred_element_type=jnp.float32)

def contract_rows(left, right):
    return lax.dot_general(left, right, (((0,), (0,)), ((), ())), preferred_element_type=jnp.float32)

def silu_parts(preact):
    sigmoid = jax.nn.sigmoid(preact)
    return (preact * sigmoid, sigmoid * (1.0 + preact * (1.0 - sigmoid)))

def norm_parts(preact):
    centred = preact - lax.optimization_barrier(jnp.mean(preact, -1, keepdims=True))
    inv_std = lax.rsqrt(lax.optimization_barrier(jnp.mean(centred * centred, -1, keepdims=True)) + EPSILON)
    return (centred * inv_std, inv_std)

def norm_back(grad_out, gain, normed, inv_std):
    scaled = grad_out * gain
    return inv_std * (scaled - lax.optimization_barrier(jnp.mean(scaled, -1, keepdims=True)) - normed * lax.optimization_barrier(jnp.mean(scaled * normed, -1, keepdims=True)))

def mlp_forward(inputs, w_first, w_hidden, biases):
    first_pre = matmul(inputs, w_first) + biases[0]
    first_act, first_slope = silu_parts(first_pre)
    first_out = first_act.astype(jnp.bfloat16)
    second_pre = matmul(first_out, w_hidden[0]) + biases[1]
    second_act, second_slope = silu_parts(second_pre)
    second_out = second_act.astype(jnp.bfloat16)
    final_pre = matmul(second_out, w_hidden[1]) + biases[2]
    return ((first_out, second_out, first_slope, second_slope), final_pre)

def mlp_back_inputs(final_grad, saved, w_first, w_hidden):
    first_out, second_out, first_slope, second_slope = saved
    final_round = final_grad.astype(jnp.bfloat16)
    second_grad = matmul(final_round, w_hidden[1].T) * second_slope
    second_round = second_grad.astype(jnp.bfloat16)
    first_grad = matmul(second_round, w_hidden[0].T) * first_slope
    first_round = first_grad.astype(jnp.bfloat16)
    input_grad = matmul(first_round, w_first.T)
    bias_grad = jnp.stack([lax.optimization_barrier(jnp.sum(first_grad, 0)), lax.optimization_barrier(jnp.sum(second_grad, 0)), lax.optimization_barrier(jnp.sum(final_grad, 0))])
    return ((first_round, second_round, final_round), bias_grad, input_grad)

def mlp_back_weights(inputs, saved, rounded):
    first_weight = contract_rows(inputs, rounded[0])
    hidden_weight = jnp.stack([contract_rows(saved[0], rounded[1]), contract_rows(saved[1], rounded[2])])
    return (first_weight, hidden_weight)

def forward_states(node_rows, ghost_rows, edge_rows, sender_ids, receiver_ids, params):
    node_count, feature_width = node_rows.shape
    full_rows = jnp.concatenate([node_rows, ghost_rows.reshape(-1, feature_width)], 0)
    edge_inputs = jnp.concatenate([edge_rows, full_rows[sender_ids], full_rows[receiver_ids]], 1)
    edge_stored_state, edge_pre = mlp_forward(edge_inputs, params[0], params[1], params[2])
    edge_normed, edge_inv = norm_parts(edge_pre)
    edge_new = (edge_normed * params[3] + params[4]).astype(jnp.bfloat16)
    aggregate = jax.ops.segment_sum(edge_new.astype(jnp.float32), receiver_ids, num_segments=node_count).astype(jnp.bfloat16)
    node_input_rows = jnp.concatenate([node_rows, aggregate], 1)
    node_saved, node_pre = mlp_forward(node_input_rows, params[5], params[6], params[7])
    node_normed, node_inv = norm_parts(node_pre)
    return ((edge_inputs, edge_stored_state, edge_normed, edge_inv), (node_input_rows, node_saved, node_normed, node_inv))

def node_backward(node_state, node_cot, params):
    node_input_rows, node_saved, node_normed, node_inv = node_state
    upstream = node_cot.astype(jnp.float32)
    gain_grad = lax.optimization_barrier(jnp.sum(upstream * node_normed, 0))
    final_grad = norm_back(upstream, params[8], node_normed, node_inv)
    rounded, bias_grad, input_grad = mlp_back_inputs(final_grad, node_saved, params[5], params[6])
    first_weight, hidden_weight = mlp_back_weights(node_input_rows, node_saved, rounded)
    return (input_grad, (first_weight, hidden_weight, bias_grad, gain_grad))

def edge_backward_inputs(edge_state, edge_cot, agg_grad, sender_ids, receiver_ids, total_rows, params):
    edge_inputs, edge_stored_state, edge_normed, edge_inv = edge_state
    feature_width = edge_cot.shape[1]
    edge_upstream = edge_cot.astype(jnp.float32)
    new_grad = edge_upstream + agg_grad[receiver_ids]
    gain_grad = lax.optimization_barrier(jnp.sum(new_grad * edge_normed, 0))
    shift_grad = lax.optimization_barrier(jnp.sum(new_grad, 0))
    final_grad = norm_back(new_grad, params[3], edge_normed, edge_inv)
    rounded, bias_grad, input_grad = mlp_back_inputs(final_grad, edge_stored_state, params[0], params[1])
    edge_grad = (edge_upstream + input_grad[:, :feature_width]).astype(jnp.bfloat16)
    full_grad = jax.ops.segment_sum(input_grad[:, feature_width:2 * feature_width], sender_ids, num_segments=total_rows)
    full_grad = full_grad + jax.ops.segment_sum(input_grad[:, 2 * feature_width:], receiver_ids, num_segments=total_rows)
    return (edge_grad, full_grad, rounded, (bias_grad, gain_grad, shift_grad))

def block_pass(node_rows, ghost_rows, edge_rows, sender_ids, receiver_ids, node_cot, edge_cot, params):
    node_count, feature_width = node_rows.shape
    total_rows = node_count + ghost_rows.shape[0] * ghost_rows.shape[1]
    edge_state, node_state = forward_states(node_rows, ghost_rows, edge_rows, sender_ids, receiver_ids, params)
    node_input_grad, node_weights = node_backward(node_state, node_cot, params)
    edge_grad, full_grad, rounded, edge_small = edge_backward_inputs(edge_state, edge_cot, node_input_grad[:, feature_width:], sender_ids, receiver_ids, total_rows, params)
    first_weight, hidden_weight = mlp_back_weights(edge_state[0], edge_state[1], rounded)
    local_grad = node_cot.astype(jnp.float32) + node_input_grad[:, :feature_width] + full_grad[:node_count]
    ghost_grad = full_grad[node_count:].reshape(ghost_rows.shape)
    weights = (first_weight, hidden_weight) + edge_small + node_weights
    return (local_grad, ghost_grad, edge_grad, weights)

def add_rows(target, rows, values):
    return target.at[rows].add(values, mode='drop')

def reference(node_latent, ghost_latent, edge_latent, senders, receivers, export_rows, node_cotangent, edge_cotangent, w_edge_in, w_edge_hidden, b_edge, gain_edge, shift_edge, w_node_in, w_node_hidden, b_node, gain_node):
    params = (w_edge_in, w_edge_hidden, b_edge, gain_edge, shift_edge, w_node_in, w_node_hidden, b_node, gain_node)
    block_count = N_GX * N_GY * N_GZ
    grid_shape = (N_GX, N_GY, N_GZ)

    def flatten(array):
        return array.reshape((block_count,) + array.shape[3:])
    stacked = tuple((flatten(array) for array in (node_latent, ghost_latent, edge_latent, senders, receivers, node_cotangent, edge_cotangent)))

    def visit(running, block_item):
        local_grad, ghost_grad, edge_grad, weights = block_pass(*block_item, params)
        return (tuple((total + term for total, term in zip(running, weights))), (local_grad, ghost_grad, edge_grad))
    start = tuple((jnp.zeros(param.shape, jnp.float32) for param in params))
    totals, (local_all, ghost_all, edge_all) = lax.scan(visit, start, stacked)
    ghost_grid = ghost_all.reshape(grid_shape + ghost_all.shape[1:])
    rows_flat = flatten(export_rows)
    node_grad = local_all
    for face_index in range(6):
        incoming = jnp.roll(ghost_grid[:, :, :, face_index], 1 - 2 * (face_index % 2), face_index // 2)
        node_grad = jax.vmap(add_rows)(node_grad, rows_flat[:, face_index], flatten(incoming))
    node_grad = node_grad.reshape(grid_shape + node_grad.shape[1:])
    edge_grad = edge_all.reshape(grid_shape + edge_all.shape[1:])
    edge_scale = EDGES ** (-0.5)
    node_scale = NODES ** (-0.5)
    return (node_grad, edge_grad, totals[0] * edge_scale, totals[1] * edge_scale, totals[2] * edge_scale, totals[3] * edge_scale, totals[4] * edge_scale, totals[5] * node_scale, totals[6] * node_scale, totals[7] * node_scale, totals[8] * node_scale)
```

```python
import functools

import jax
import jax.numpy as jnp
from jax import lax
from jax.experimental import pallas as pl
from jax.experimental.pallas import tpu as pltpu
from jax.sharding import PartitionSpec as P

EPSILON = 1e-05
MESH = pl.DeviceIdType.MESH
BF = jnp.bfloat16
F32 = jnp.float32
D = 128
NODES = 512
FACES = 6
SLOTS = 64
FULL = NODES + FACES * SLOTS
EDGES = 2816
CH = 256
CHUNKS = EDGES // CH
SEND_TILES = FULL // D
RECV_TILES = NODES // D
TILES = SEND_TILES + RECV_TILES
PIECES = 32
PIECE = 40
ROW_EW1 = 0
ROW_EWH = 384
ROW_ESM = 640
ROW_NW1 = 648
ROW_NWH = 904
ROW_NSM = 1160
ROWS = PIECES * PIECE


def mm(a, b):
    return jnp.dot(a, b, preferred_element_type=F32)


def mm_tn(a, b):
    return lax.dot_general(a, b, (((0,), (0,)), ((), ())), preferred_element_type=F32)


def transposed(w):
    return w.astype(F32).T.astype(BF)


def silu_parts(p):
    s = 0.5 * jnp.tanh(0.5 * p) + 0.5
    z = p * s
    return z, s + z * (1.0 - s)


def norm_parts(p):
    c = p - jnp.mean(p, -1, keepdims=True)
    inv = lax.rsqrt(jnp.mean(c * c, -1, keepdims=True) + EPSILON)
    return c * inv, inv


def norm_back(u, gain, n, inv):
    t = u * gain
    return inv * (t - jnp.mean(t, -1, keepdims=True) - n * jnp.mean(t * n, -1, keepdims=True))


def fold(x):
    return jnp.sum(x.reshape(x.shape[0] // 8, 8, x.shape[1]), 0)


def row_sum(x):
    return jnp.sum(fold(x), 0, keepdims=True)


def column_digits(ids_row):
    lo, hi = [], []
    for j in range(ids_row.shape[1] // D):
        t = jnp.broadcast_to(ids_row[:, j * D : (j + 1) * D], (D, D)).T
        lo.append((t & (D - 1)).astype(F32).astype(BF))
        hi.append((t >> 7).astype(F32).astype(BF))
    return jnp.concatenate(lo, 0), jnp.concatenate(hi, 0)


def one_hot_columns(lo, hi, tiles):
    lane = lax.broadcasted_iota(jnp.int32, lo.shape, 1).astype(F32).astype(BF)
    zero = jnp.zeros(lo.shape, BF)
    base = jnp.where(lo == lane, jnp.ones(lo.shape, BF), zero)
    return [jnp.where(hi == BF(k), base, zero) for k in range(tiles)]


def one_hot_rows(ids_row, tiles):
    n = ids_row.shape[1]
    lo = jnp.broadcast_to((ids_row & (D - 1)).astype(F32), (D, n)).astype(BF)
    hi = jnp.broadcast_to((ids_row >> 7).astype(F32), (D, n)).astype(BF)
    row = lax.broadcasted_iota(jnp.int32, (D, n), 0).astype(F32).astype(BF)
    zero = jnp.zeros((D, n), BF)
    base = jnp.where(lo == row, jnp.ones((D, n), BF), zero)
    return [jnp.where(hi == BF(k), base, zero) for k in range(tiles)]


def compute_kernel(
    scales,
    node_ref, ghost_ref, edge_ref, send_ref, recv_ref, ncot_ref, ecot_ref,
    ew1_ref, ewh_ref, eb_ref, eg_ref, es_ref, nw1_ref, nwh_ref, nb_ref, ng_ref,
    local_ref, ghost_out_ref, edge_out_ref, pack_ref,
    table, z1, z2, sl1, sl2, nrm, inv, rlo, rhi, agg, acc, w3t, w2t, w1t, aggb, small,
):
    edge_scale, node_scale = scales
    node = node_ref[0, 0, 0]
    ghosts = ghost_ref[0, 0, 0].reshape(FACES * SLOTS, D)
    full = jnp.concatenate([node, ghosts], 0)
    table[0:FULL] = mm(full, ew1_ref[D : 2 * D]).astype(BF)
    table[FULL : FULL + NODES] = mm(node, ew1_ref[2 * D : 3 * D]).astype(BF)
    table[FULL + NODES :] = ew1_ref[0:D]
    w3t[...] = transposed(ewh_ref[1])
    w2t[...] = transposed(ewh_ref[0])
    w1t[...] = transposed(ew1_ref[0:D])
    agg[...] = jnp.zeros_like(agg)
    acc[...] = jnp.zeros_like(acc)
    small[...] = jnp.zeros_like(small)
    pack_ref[...] = jnp.zeros_like(pack_ref)
    egain = eg_ref[...].reshape(1, D)
    eshift = es_ref[...].reshape(1, D)

    def forward(i, carry):
        off = pl.multiple_of(i * CH, CH)
        rows = pl.ds(off, CH)
        s_row = send_ref[0, 0, :, rows]
        r_row = recv_ref[0, 0, :, rows]
        slo, shi = column_digits(s_row)
        lo, hi = column_digits(r_row)
        rlo[rows] = lo
        rhi[rows] = hi
        hot = one_hot_columns(slo, shi, SEND_TILES) + one_hot_columns(lo, hi, RECV_TILES)
        lhs = jnp.concatenate(hot + [edge_ref[0, 0, 0, rows]], 1)
        p1 = mm(lhs, table[...]) + eb_ref[0:1]
        a1, d1 = silu_parts(p1)
        b1 = a1.astype(BF)
        z1[rows] = b1
        sl1[rows] = d1
        p2 = mm(b1, ewh_ref[0]) + eb_ref[1:2]
        a2, d2 = silu_parts(p2)
        b2 = a2.astype(BF)
        z2[rows] = b2
        sl2[rows] = d2
        q = mm(b2, ewh_ref[1]) + eb_ref[2:3]
        n, iv = norm_parts(q)
        nrm[rows] = n
        inv[rows] = jnp.broadcast_to(iv, (CH, D))
        new = (n * egain + eshift).astype(BF)
        hot_t = jnp.concatenate(one_hot_rows(r_row, RECV_TILES), 0)
        agg[...] += mm(hot_t, new)
        return carry

    lax.fori_loop(0, CHUNKS, forward, 0)

    ngain = ng_ref[...].reshape(1, D)
    node_in = jnp.concatenate([node, agg[...].astype(BF)], 1)
    a1, d1 = silu_parts(mm(node_in, nw1_ref[...]) + nb_ref[0:1])
    b1 = a1.astype(BF)
    a2, d2 = silu_parts(mm(b1, nwh_ref[0]) + nb_ref[1:2])
    b2 = a2.astype(BF)
    n, iv = norm_parts(mm(b2, nwh_ref[1]) + nb_ref[2:3])
    u = ncot_ref[0, 0, 0].astype(F32)
    g3 = norm_back(u, ngain, n, iv)
    h3 = g3.astype(BF)
    g2 = mm(h3, transposed(nwh_ref[1])) * d2
    h2 = g2.astype(BF)
    g1 = mm(h2, transposed(nwh_ref[0])) * d1
    h1 = g1.astype(BF)
    local_ref[...] = u + mm(h1, transposed(nw1_ref[0:D]))
    aggb[...] = mm(h1, transposed(nw1_ref[D : 2 * D])).astype(BF)
    pack_ref[ROW_NW1 : ROW_NW1 + 2 * D] = mm_tn(node_in, h1) * node_scale
    pack_ref[ROW_NWH : ROW_NWH + D] = mm_tn(b1, h2) * node_scale
    pack_ref[ROW_NWH + D : ROW_NWH + 2 * D] = mm_tn(b2, h3) * node_scale
    pack_ref[ROW_NSM : ROW_NSM + 4] = node_scale * jnp.concatenate(
        [row_sum(g1), row_sum(g2), row_sum(g3), row_sum(u * n)], 0
    )

    def backward(i, carry):
        off = pl.multiple_of(i * CH, CH)
        rows = pl.ds(off, CH)
        s_row = send_ref[0, 0, :, rows]
        r_row = recv_ref[0, 0, :, rows]
        hot = jnp.concatenate(one_hot_columns(rlo[rows], rhi[rows], RECV_TILES), 1)
        cot = ecot_ref[0, 0, 0, rows].astype(F32)
        u = cot + mm(hot, aggb[...])
        n = nrm[rows]
        g3 = norm_back(u, egain, n, inv[rows])
        h3 = g3.astype(BF)
        g2 = mm(h3, w3t[...]) * sl2[rows]
        h2 = g2.astype(BF)
        g1 = mm(h2, w2t[...]) * sl1[rows]
        h1 = g1.astype(BF)
        edge_out_ref[0, 0, 0, rows] = (cot + mm(h1, w1t[...])).astype(BF)
        pack_ref[ROW_EW1 : ROW_EW1 + D] += mm_tn(edge_ref[0, 0, 0, rows], h1)
        pack_ref[ROW_EWH : ROW_EWH + D] += mm_tn(z1[rows], h2)
        pack_ref[ROW_EWH + D : ROW_EWH + 2 * D] += mm_tn(z2[rows], h3)
        hot_t = jnp.concatenate(one_hot_rows(s_row, SEND_TILES) + one_hot_rows(r_row, RECV_TILES), 0)
        acc[...] += mm(hot_t, h1)
        small[0] += fold(g1)
        small[1] += fold(g2)
        small[2] += fold(g3)
        small[3] += fold(u * n)
        small[4] += fold(u)
        return carry

    lax.fori_loop(0, CHUNKS, backward, 0)

    sums = acc[0:FULL].astype(BF)
    sums_r = acc[FULL : FULL + NODES].astype(BF)
    back = mm(sums, transposed(ew1_ref[D : 2 * D]))
    local_ref[...] += back[0:NODES] + mm(sums_r, transposed(ew1_ref[2 * D : 3 * D]))
    ghost_out_ref[...] = back[NODES:].reshape(FACES, SLOTS, D)
    pack_ref[ROW_EW1 : ROW_EW1 + D] = pack_ref[ROW_EW1 : ROW_EW1 + D] * edge_scale
    pack_ref[ROW_EW1 + D : ROW_EW1 + 2 * D] = mm_tn(full, sums) * edge_scale
    pack_ref[ROW_EW1 + 2 * D : ROW_EW1 + 3 * D] = mm_tn(node, sums_r) * edge_scale
    pack_ref[ROW_EWH : ROW_EWH + 2 * D] = pack_ref[ROW_EWH : ROW_EWH + 2 * D] * edge_scale
    pack_ref[ROW_ESM : ROW_ESM + 5] = edge_scale * jnp.concatenate(
        [jnp.sum(small[j], 0, keepdims=True) for j in range(5)], 0
    )


VMEM = pl.BlockSpec(memory_space=pltpu.VMEM)


def local_compute(args, scales):
    return pl.pallas_call(
        functools.partial(compute_kernel, scales),
        out_shape=(
            jax.ShapeDtypeStruct((NODES, D), F32),
            jax.ShapeDtypeStruct((FACES, SLOTS, D), F32),
            jax.ShapeDtypeStruct((1, 1, 1, EDGES, D), BF),
            jax.ShapeDtypeStruct((ROWS, D), F32),
        ),
        in_specs=[VMEM] * len(args),
        out_specs=(VMEM,) * 4,
        scratch_shapes=[
            pltpu.VMEM((FULL + NODES + D, D), BF),
            pltpu.VMEM((EDGES, D), BF),
            pltpu.VMEM((EDGES, D), BF),
            pltpu.VMEM((EDGES, D), F32),
            pltpu.VMEM((EDGES, D), F32),
            pltpu.VMEM((EDGES, D), F32),
            pltpu.VMEM((EDGES, D), F32),
            pltpu.VMEM((EDGES, D), BF),
            pltpu.VMEM((EDGES, D), BF),
            pltpu.VMEM((NODES, D), F32),
            pltpu.VMEM((FULL + NODES, D), F32),
            pltpu.VMEM((D, D), BF),
            pltpu.VMEM((D, D), BF),
            pltpu.VMEM((D, D), BF),
            pltpu.VMEM((NODES, D), BF),
            pltpu.VMEM((5, 8, D), F32),
        ],
        compiler_params=pltpu.CompilerParams(vmem_limit_bytes=48 * 2**20),
        cost_estimate=pl.CostEstimate(flops=6_000_000_000, bytes_accessed=6_000_000, transcendentals=800_000),
    )(*args)


def comm_kernel(
    pack_ref, ghost_ref, local_ref, rows_ref,
    out_ref, node_ref,
    pair_buf, half, plane_buf, zbuf, fin, gbuf,
    pair_s, pair_r, plane_s, plane_r, z_s, z_r, ag_s, ag_r, back_s, back_r, g_s, g_r,
):
    gx, gy, gz = lax.axis_index("gx"), lax.axis_index("gy"), lax.axis_index("gz")
    y, zl = gx // 2, gx % 2
    x, c = gz // 2, gz % 2
    z = gy * 2 + zl
    plane = x * 4 + y
    sibling = (gx, gy, gz + 1 - 2 * c)

    def plane_peer(d):
        px, py = (x + d // 4) % 4, (y + d % 4) % 4
        return px * 4 + py, (py * 2 + zl, gy, px * 2 + c)

    def z_peer(d):
        pz = (z + d) % 8
        return (y * 2 + pz % 2, pz // 2, gz)

    ghost_to = []
    for f in range(FACES):
        step = 1 if f % 2 == 0 else -1
        ghost_to.append((
            ((gx + step + 8) % 8, gy, gz),
            (gx, (gy + step + 4) % 4, gz),
            (gx, gy, (gz + step + 8) % 8),
        )[f // 2])

    plane_order = [10, 9, 11, 6, 14, 2, 8, 5, 7, 13, 15, 1, 3, 4, 12]
    z_order = [4, 3, 5, 2, 6, 1, 7]

    barrier = pltpu.get_barrier_semaphore()
    peers = [sibling] + [plane_peer(d)[1] for d in plane_order] + [z_peer(d) for d in z_order] + ghost_to
    for peer in peers:
        pl.semaphore_signal(barrier, inc=1, device_id=peer, device_id_type=MESH)
    pl.semaphore_wait(barrier, len(peers))

    def remote(src, dst, send, recv, peer):
        return pltpu.make_async_remote_copy(
            src_ref=src, dst_ref=dst, send_sem=send, recv_sem=recv, device_id=peer, device_id_type=MESH
        )

    pair = remote(pack_ref.at[pl.ds((1 - c) * 16, 16)], pair_buf, pair_s, pair_r, sibling)
    pair.start()
    ghost_copies = []
    for f in range(FACES):
        cp = remote(ghost_ref.at[f], gbuf.at[f], g_s.at[f], g_r.at[f], ghost_to[f])
        cp.start()
        ghost_copies.append(cp)
    pair.wait_recv()
    half[...] = pack_ref[pl.ds(c * 16, 16)] + pair_buf[...]

    copies = []
    for d in plane_order:
        index, peer = plane_peer(d)
        cp = remote(half.at[index], plane_buf.at[d], plane_s.at[d], plane_r.at[d], peer)
        cp.start()
        copies.append(cp)

    total = local_ref[...]
    for f in range(FACES):
        ghost_copies[f].wait_recv()
        got = gbuf[f]
        high = got.astype(BF)
        low = (got - high.astype(F32)).astype(BF)
        ids = jnp.broadcast_to(rows_ref[f : f + 1], (NODES, SLOTS))
        hot = jnp.where(ids == lax.broadcasted_iota(jnp.int32, (NODES, SLOTS), 0), 1.0, 0.0).astype(BF)
        total = total + (mm(hot, high) + mm(hot, low))
    node_ref[...] = total

    own = half[plane]
    for cp in copies:
        cp.wait_recv()
    for d in range(1, 16):
        own = own + plane_buf[d]
    zbuf[z] = own
    z_copies = []
    for d in z_order:
        cp = remote(zbuf.at[z], zbuf.at[z], z_s.at[d], z_r.at[d], z_peer(d))
        cp.start()
        z_copies.append(cp)
    for cp in z_copies:
        cp.wait_recv()
    own = zbuf[0]
    for d in range(1, 8):
        own = own + zbuf[d]
    mine = c * 16 + plane
    fin[mine] = own

    gathers = []
    for d in plane_order:
        _, peer = plane_peer(d)
        cp = remote(fin.at[mine], fin.at[mine], ag_s.at[d], ag_r.at[d], peer)
        cp.start()
        gathers.append(cp)
    backs = []
    cp = remote(fin.at[mine], fin.at[mine], back_s.at[0], back_r.at[0], sibling)
    cp.start()
    backs.append(cp)
    for d, cp in reversed(list(zip(plane_order, gathers))):
        cp.wait_recv()
        source = c * 16 + plane_peer(16 - d if d % 4 == 0 else (4 - d // 4) % 4 * 4 + 4 - d % 4)[0]
        cp = remote(fin.at[source], fin.at[source], back_s.at[d], back_r.at[d], sibling)
        cp.start()
        backs.append(cp)
    for cp in backs:
        cp.wait_recv()
    out_ref[...] = fin[...]

    pair.wait_send()
    for cp in ghost_copies + copies + z_copies + gathers + backs:
        cp.wait_send()


def exchange(pack, ghost, local, rows):
    return pl.pallas_call(
        comm_kernel,
        out_shape=(
            jax.ShapeDtypeStruct((PIECES, PIECE, D), F32),
            jax.ShapeDtypeStruct((NODES, D), F32),
        ),
        in_specs=[VMEM] * 4,
        out_specs=(VMEM,) * 2,
        scratch_shapes=[
            pltpu.VMEM((16, PIECE, D), F32),
            pltpu.VMEM((16, PIECE, D), F32),
            pltpu.VMEM((16, PIECE, D), F32),
            pltpu.VMEM((8, PIECE, D), F32),
            pltpu.VMEM((PIECES, PIECE, D), F32),
            pltpu.VMEM((FACES, SLOTS, D), F32),
            pltpu.SemaphoreType.DMA,
            pltpu.SemaphoreType.DMA,
            pltpu.SemaphoreType.DMA((16,)),
            pltpu.SemaphoreType.DMA((16,)),
            pltpu.SemaphoreType.DMA((8,)),
            pltpu.SemaphoreType.DMA((8,)),
            pltpu.SemaphoreType.DMA((16,)),
            pltpu.SemaphoreType.DMA((16,)),
            pltpu.SemaphoreType.DMA((16,)),
            pltpu.SemaphoreType.DMA((16,)),
            pltpu.SemaphoreType.DMA((6,)),
            pltpu.SemaphoreType.DMA((6,)),
        ],
        compiler_params=pltpu.CompilerParams(collective_id=0, has_side_effects=True, vmem_limit_bytes=24 * 2**20),
        cost_estimate=pl.CostEstimate(flops=300_000_000, bytes_accessed=2_000_000, transcendentals=0),
    )(pack, ghost, local, rows)


def unpack_kernel(pack_ref, node_in, node_out, ew1, ewh, eb, eg, es, nw1, nwh, nb, ng):
    node_out[0, 0, 0] = node_in[...]
    ew1[...] = pack_ref[ROW_EW1 : ROW_EW1 + 3 * D]
    ewh[0] = pack_ref[ROW_EWH : ROW_EWH + D]
    ewh[1] = pack_ref[ROW_EWH + D : ROW_EWH + 2 * D]
    nw1[...] = pack_ref[ROW_NW1 : ROW_NW1 + 2 * D]
    nwh[0] = pack_ref[ROW_NWH : ROW_NWH + D]
    nwh[1] = pack_ref[ROW_NWH + D : ROW_NWH + 2 * D]
    eb[...] = pack_ref[ROW_ESM : ROW_ESM + 3]
    eg[...] = pack_ref[ROW_ESM + 3 : ROW_ESM + 4].reshape(D)
    es[...] = pack_ref[ROW_ESM + 4 : ROW_ESM + 5].reshape(D)
    nb[...] = pack_ref[ROW_NSM : ROW_NSM + 3]
    ng[...] = pack_ref[ROW_NSM + 3 : ROW_NSM + 4].reshape(D)


def unpack(pack, node):
    shapes = ((1, 1, 1, NODES, D), (3 * D, D), (2, D, D), (3, D), (D,), (D,), (2 * D, D), (2, D, D), (3, D), (D,))
    return pl.pallas_call(
        unpack_kernel,
        out_shape=tuple(jax.ShapeDtypeStruct(s, F32) for s in shapes),
        in_specs=[VMEM] * 2,
        out_specs=(VMEM,) * len(shapes),
        compiler_params=pltpu.CompilerParams(vmem_limit_bytes=8 * 2**20),
        cost_estimate=pl.CostEstimate(flops=1_000_000, bytes_accessed=2_000_000, transcendentals=0),
    )(pack, node)


def on_device(
    node_latent, ghost_latent, edge_latent, senders, receivers, export_rows, node_cotangent, edge_cotangent,
    w_edge_in, w_edge_hidden, b_edge, gain_edge, shift_edge, w_node_in, w_node_hidden, b_node, gain_node,
):
    devices = lax.axis_size("gx") * lax.axis_size("gy") * lax.axis_size("gz")
    scales = (float(EDGES * devices) ** (-0.5), float(NODES * devices) ** (-0.5))
    local, ghost, edge_grad, pack = local_compute(
        (
            node_latent, ghost_latent, edge_latent, senders, receivers, node_cotangent, edge_cotangent,
            w_edge_in, w_edge_hidden, b_edge, gain_edge, shift_edge, w_node_in, w_node_hidden, b_node, gain_node,
        ),
        scales,
    )
    summed, node = exchange(pack.reshape(PIECES, PIECE, D), ghost, local, export_rows.reshape(FACES, SLOTS))
    out = unpack(summed.reshape(ROWS, D), node)
    return (out[0], edge_grad) + tuple(out[1:])


def solution(mesh):
    block = lambda dims: P("gx", "gy", "gz", *([None] * dims))
    in_specs = tuple(block(k) for k in (2, 3, 2, 1, 1, 2, 2, 2)) + (P(),) * 9
    out_specs = (block(2), block(2)) + (P(),) * 9
    return jax.shard_map(on_device, mesh=mesh, in_specs=in_specs, out_specs=out_specs, check_vma=False)
```

```python
import functools

import jax
import jax.numpy as jnp
from jax import lax
from jax.experimental import pallas as pl
from jax.experimental.pallas import tpu as pltpu
from jax.sharding import PartitionSpec as P

EPSILON = 1e-05
MESH = pl.DeviceIdType.MESH
BF = jnp.bfloat16
F32 = jnp.float32
D = 128
NODES = 512
FACES = 6
SLOTS = 64
FULL = NODES + FACES * SLOTS
EDGES = 2816
CH = 1408
CHUNKS = EDGES // CH
SEND_TILES = FULL // D
RECV_TILES = NODES // D
TILES = SEND_TILES + RECV_TILES
PIECES = 32
PIECE = 40
ROW_EW1 = 0
ROW_EWH = 384
ROW_ESM = 640
ROW_NW1 = 648
ROW_NWH = 904
ROW_NSM = 1160
ROWS = PIECES * PIECE
PLANE_ORDER = (10, 9, 11, 6, 14, 2, 8, 5, 7, 13, 15, 1, 3, 4, 12)
Z_ORDER = (4, 3, 5, 2, 6, 1, 7)


def mm(a, b):
    return jnp.dot(a, b, preferred_element_type=F32)


def mm_tn(a, b):
    return lax.dot_general(a, b, (((0,), (0,)), ((), ())), preferred_element_type=F32)


def transposed(w):
    return w.astype(F32).T.astype(BF)


def silu_parts(p):
    s = 0.5 * jnp.tanh(0.5 * p) + 0.5
    z = p * s
    return z, s + z * (1.0 - s)


def norm_parts(p):
    c = p - jnp.mean(p, -1, keepdims=True)
    inv = lax.rsqrt(jnp.mean(c * c, -1, keepdims=True) + EPSILON)
    return c * inv, inv


def norm_back(u, gain, n, inv):
    t = u * gain
    return inv * (t - jnp.mean(t, -1, keepdims=True) - n * jnp.mean(t * n, -1, keepdims=True))


def fold(x):
    return jnp.sum(x.reshape(x.shape[0] // 8, 8, x.shape[1]), 0)


def row_sum(x):
    return jnp.sum(fold(x), 0, keepdims=True)


def column_digits(ids_row):
    lo, hi = [], []
    for j in range(ids_row.shape[1] // D):
        t = jnp.broadcast_to(ids_row[:, j * D : (j + 1) * D], (D, D)).T
        lo.append((t & (D - 1)).astype(F32).astype(BF))
        hi.append((t >> 7).astype(F32).astype(BF))
    return jnp.concatenate(lo, 0), jnp.concatenate(hi, 0)


def one_hot_columns(lo, hi, tiles):
    lane = lax.broadcasted_iota(jnp.int32, lo.shape, 1).astype(F32).astype(BF)
    zero = jnp.zeros(lo.shape, BF)
    base = jnp.where(lo == lane, jnp.ones(lo.shape, BF), zero)
    return [jnp.where(hi == BF(k), base, zero) for k in range(tiles)]


def one_hot_rows(ids_row, tiles):
    n = ids_row.shape[1]
    lo = jnp.broadcast_to((ids_row & (D - 1)).astype(F32), (D, n)).astype(BF)
    hi = jnp.broadcast_to((ids_row >> 7).astype(F32), (D, n)).astype(BF)
    row = lax.broadcasted_iota(jnp.int32, (D, n), 0).astype(F32).astype(BF)
    zero = jnp.zeros((D, n), BF)
    base = jnp.where(lo == row, jnp.ones((D, n), BF), zero)
    return [jnp.where(hi == BF(k), base, zero) for k in range(tiles)]


class Exchange:
    def __init__(self, refs):
        (
            self.pack, self.pair_buf, self.half, self.plane_buf, self.zbuf, self.fin, self.gbuf,
            self.pair_s, self.pair_r, self.plane_s, self.plane_r, self.z_s, self.z_r,
            self.ag_s, self.ag_r, self.back_s, self.back_r, self.g_s, self.g_r,
        ) = refs
        gx, gy, gz = lax.axis_index("gx"), lax.axis_index("gy"), lax.axis_index("gz")
        self.y, self.zl = gx // 2, gx % 2
        self.x, self.c = gz // 2, gz % 2
        self.z = gy * 2 + self.zl
        self.at = (gx, gy, gz)
        self.plane = self.x * 4 + self.y
        self.sibling = (gx, gy, gz + 1 - 2 * self.c)
        self.started = []
        self.ghost_to = []
        for f in range(FACES):
            step = 1 if f % 2 == 0 else -1
            self.ghost_to.append((
                ((gx + step + 8) % 8, gy, gz),
                (gx, (gy + step + 4) % 4, gz),
                (gx, gy, (gz + step + 8) % 8),
            )[f // 2])

    def plane_peer(self, d):
        px, py = (self.x + d // 4) % 4, (self.y + d % 4) % 4
        return px * 4 + py, (py * 2 + self.zl, self.at[1], px * 2 + self.c)

    def z_peer(self, d):
        pz = (self.z + d) % 8
        return (self.y * 2 + pz % 2, pz // 2, self.at[2])

    def greet(self):
        barrier = pltpu.get_barrier_semaphore()
        peers = [self.sibling] + [self.plane_peer(d)[1] for d in PLANE_ORDER]
        peers += [self.z_peer(d) for d in Z_ORDER] + self.ghost_to
        for peer in peers:
            pl.semaphore_signal(barrier, inc=1, device_id=peer, device_id_type=MESH)
        self.greeted = len(peers)

    def remote(self, src, dst, send, recv, peer):
        cp = pltpu.make_async_remote_copy(
            src_ref=src, dst_ref=dst, send_sem=send, recv_sem=recv, device_id=peer, device_id_type=MESH
        )
        cp.start()
        self.started.append(cp)
        return cp

    def swap_halves(self):
        pl.semaphore_wait(pltpu.get_barrier_semaphore(), self.greeted)
        self.pair = self.remote(
            self.pack.at[pl.ds((1 - self.c) * 16, 16)], self.pair_buf, self.pair_s, self.pair_r, self.sibling
        )

    def reduce_in_plane(self):
        self.pair.wait_recv()
        self.half[...] = self.pack[pl.ds(self.c * 16, 16)] + self.pair_buf[...]
        self.in_plane = []
        for d in PLANE_ORDER:
            index, peer = self.plane_peer(d)
            self.in_plane.append(
                self.remote(self.half.at[index], self.plane_buf.at[d], self.plane_s.at[d], self.plane_r.at[d], peer)
            )

    def send_ghosts(self, ghost_ref):
        self.ghosts = [
            self.remote(ghost_ref.at[f], self.gbuf.at[f], self.g_s.at[f], self.g_r.at[f], self.ghost_to[f])
            for f in range(FACES)
        ]

    def reduce_along_z(self):
        own = self.half[self.plane]
        for cp in self.in_plane:
            cp.wait_recv()
        for d in range(1, 16):
            own = own + self.plane_buf[d]
        self.zbuf[self.z] = own
        self.along_z = [
            self.remote(self.zbuf.at[self.z], self.zbuf.at[self.z], self.z_s.at[d], self.z_r.at[d], self.z_peer(d))
            for d in Z_ORDER
        ]

    def add_ghosts(self, total, rows_ref):
        for f in range(FACES):
            self.ghosts[f].wait_recv()
            got = self.gbuf[f]
            high = got.astype(BF)
            low = (got - high.astype(F32)).astype(BF)
            ids = jnp.broadcast_to(rows_ref[f], (NODES, SLOTS))
            hot = jnp.where(ids == lax.broadcasted_iota(jnp.int32, (NODES, SLOTS), 0), 1.0, 0.0).astype(BF)
            total = total + (mm(hot, high) + mm(hot, low))
        return total

    def spread(self):
        for cp in self.along_z:
            cp.wait_recv()
        own = self.zbuf[0]
        for d in range(1, 8):
            own = own + self.zbuf[d]
        mine = self.c * 16 + self.plane
        self.fin[mine] = own
        piece = self.fin.at[mine]
        gathers = [
            self.remote(piece, piece, self.ag_s.at[d], self.ag_r.at[d], self.plane_peer(d)[1]) for d in PLANE_ORDER
        ]
        backs = [self.remote(piece, piece, self.back_s.at[0], self.back_r.at[0], self.sibling)]
        for d, cp in reversed(list(zip(PLANE_ORDER, gathers))):
            cp.wait_recv()
            source = (4 - d // 4) % 4 * 4 + (4 - d % 4) % 4
            piece = self.fin.at[self.c * 16 + self.plane_peer(source)[0]]
            backs.append(self.remote(piece, piece, self.back_s.at[d], self.back_r.at[d], self.sibling))
        for cp in backs:
            cp.wait_recv()

    def drain(self):
        for cp in self.started:
            cp.wait_send()


def fused_kernel(scales, *refs):
    inputs, refs = refs[:INPUTS], refs[INPUTS:]
    edge_out_ref, out_ref, node_out_ref = refs[:3]
    held, refs = refs[3 : 3 + INPUTS], refs[3 + INPUTS :]
    in_sem = refs[0]
    (
        table, z1, z2, sl1, sl2, nrm, inv, rlo, rhi, agg, acc, w3t, w2t, w1t, aggb, small,
        local_ref, ghost_out_ref, pack_ref,
    ) = refs[1:20]
    comm_refs = refs[20:]
    loads = [pltpu.make_async_copy(a, b, in_sem.at[k]) for k, (a, b) in enumerate(zip(inputs, held))]
    for cp in loads:
        cp.start()
    comm = Exchange(comm_refs)
    comm.greet()
    (
        node_ref, ghost_ref, ew1_ref, ewh_ref, send_ref, recv_ref, edge_ref, eb_ref, eg_ref, es_ref,
        nw1_ref, nwh_ref, nb_ref, ng_ref, ncot_ref, ecot_ref, rows_ref,
    ) = held
    edge_scale, node_scale = scales
    for cp in loads[:4]:
        cp.wait()
    node = node_ref[0, 0, 0]
    ghosts = ghost_ref[0, 0, 0].reshape(FACES * SLOTS, D)
    full = jnp.concatenate([node, ghosts], 0)
    table[0:FULL] = mm(full, ew1_ref[D : 2 * D]).astype(BF)
    table[FULL : FULL + NODES] = mm(node, ew1_ref[2 * D : 3 * D]).astype(BF)
    table[FULL + NODES :] = ew1_ref[0:D]
    w3t[...] = transposed(ewh_ref[1])
    w2t[...] = transposed(ewh_ref[0])
    w1t[...] = transposed(ew1_ref[0:D])
    agg[...] = jnp.zeros_like(agg)
    acc[...] = jnp.zeros_like(acc)
    small[...] = jnp.zeros_like(small)
    pack_ref[...] = jnp.zeros_like(pack_ref)
    for cp in loads[4:10]:
        cp.wait()
    egain = eg_ref[...].reshape(1, D)
    eshift = es_ref[...].reshape(1, D)

    def forward(i, carry):
        off = pl.multiple_of(i * CH, CH)
        rows = pl.ds(off, CH)
        s_row = send_ref[0, 0, :, rows]
        r_row = recv_ref[0, 0, :, rows]
        slo, shi = column_digits(s_row)
        lo, hi = column_digits(r_row)
        rlo[rows] = lo
        rhi[rows] = hi
        hot = one_hot_columns(slo, shi, SEND_TILES) + one_hot_columns(lo, hi, RECV_TILES)
        lhs = jnp.concatenate(hot + [edge_ref[0, 0, 0, rows]], 1)
        p1 = mm(lhs, table[...]) + eb_ref[0:1]
        a1, d1 = silu_parts(p1)
        b1 = a1.astype(BF)
        z1[rows] = b1
        sl1[rows] = d1
        p2 = mm(b1, ewh_ref[0]) + eb_ref[1:2]
        a2, d2 = silu_parts(p2)
        b2 = a2.astype(BF)
        z2[rows] = b2
        sl2[rows] = d2
        q = mm(b2, ewh_ref[1]) + eb_ref[2:3]
        n, iv = norm_parts(q)
        nrm[rows] = n
        inv[rows] = jnp.broadcast_to(iv, (CH, D))
        new = (n * egain + eshift).astype(BF)
        hot_t = jnp.concatenate(one_hot_rows(r_row, RECV_TILES), 0)
        agg[...] += mm(hot_t, new)
        return carry

    lax.fori_loop(0, CHUNKS, forward, 0)

    for cp in loads[10:]:
        cp.wait()
    ngain = ng_ref[...].reshape(1, D)
    node_in = jnp.concatenate([node, agg[...].astype(BF)], 1)
    a1, d1 = silu_parts(mm(node_in, nw1_ref[...]) + nb_ref[0:1])
    b1 = a1.astype(BF)
    a2, d2 = silu_parts(mm(b1, nwh_ref[0]) + nb_ref[1:2])
    b2 = a2.astype(BF)
    n, iv = norm_parts(mm(b2, nwh_ref[1]) + nb_ref[2:3])
    u = ncot_ref[0, 0, 0].astype(F32)
    g3 = norm_back(u, ngain, n, iv)
    h3 = g3.astype(BF)
    g2 = mm(h3, transposed(nwh_ref[1])) * d2
    h2 = g2.astype(BF)
    g1 = mm(h2, transposed(nwh_ref[0])) * d1
    h1 = g1.astype(BF)
    local_ref[...] = u + mm(h1, transposed(nw1_ref[0:D]))
    aggb[...] = mm(h1, transposed(nw1_ref[D : 2 * D])).astype(BF)
    pack_ref[ROW_NW1 : ROW_NW1 + 2 * D] = mm_tn(node_in, h1) * node_scale
    pack_ref[ROW_NWH : ROW_NWH + D] = mm_tn(b1, h2) * node_scale
    pack_ref[ROW_NWH + D : ROW_NWH + 2 * D] = mm_tn(b2, h3) * node_scale
    pack_ref[ROW_NSM : ROW_NSM + 4] = node_scale * jnp.concatenate(
        [row_sum(g1), row_sum(g2), row_sum(g3), row_sum(u * n)], 0
    )

    def backward(i, carry):
        off = pl.multiple_of(i * CH, CH)
        rows = pl.ds(off, CH)
        s_row = send_ref[0, 0, :, rows]
        r_row = recv_ref[0, 0, :, rows]
        hot = jnp.concatenate(one_hot_columns(rlo[rows], rhi[rows], RECV_TILES), 1)
        cot = ecot_ref[0, 0, 0, rows].astype(F32)
        u = cot + mm(hot, aggb[...])
        n = nrm[rows]
        g3 = norm_back(u, egain, n, inv[rows])
        h3 = g3.astype(BF)
        g2 = mm(h3, w3t[...]) * sl2[rows]
        h2 = g2.astype(BF)
        g1 = mm(h2, w2t[...]) * sl1[rows]
        h1 = g1.astype(BF)
        edge_out_ref[0, 0, 0, rows] = (cot + mm(h1, w1t[...])).astype(BF)
        pack_ref[ROW_EW1 : ROW_EW1 + D] += mm_tn(edge_ref[0, 0, 0, rows], h1)
        pack_ref[ROW_EWH : ROW_EWH + D] += mm_tn(z1[rows], h2)
        pack_ref[ROW_EWH + D : ROW_EWH + 2 * D] += mm_tn(z2[rows], h3)
        hot_t = jnp.concatenate(one_hot_rows(s_row, SEND_TILES) + one_hot_rows(r_row, RECV_TILES), 0)
        acc[...] += mm(hot_t, h1)
        small[0] += fold(g1)
        small[1] += fold(g2)
        small[2] += fold(g3)
        small[3] += fold(u * n)
        small[4] += fold(u)
        return carry

    lax.fori_loop(0, CHUNKS, backward, 0)

    sums = acc[0:FULL].astype(BF)
    sums_r = acc[FULL : FULL + NODES].astype(BF)
    pack_ref[ROW_EW1 : ROW_EW1 + D] = pack_ref[ROW_EW1 : ROW_EW1 + D] * edge_scale
    pack_ref[ROW_EW1 + D : ROW_EW1 + 2 * D] = mm_tn(full, sums) * edge_scale
    pack_ref[ROW_EW1 + 2 * D : ROW_EW1 + 3 * D] = mm_tn(node, sums_r) * edge_scale
    pack_ref[ROW_EWH : ROW_EWH + 2 * D] = pack_ref[ROW_EWH : ROW_EWH + 2 * D] * edge_scale
    pack_ref[ROW_ESM : ROW_ESM + 5] = edge_scale * jnp.concatenate(
        [jnp.sum(small[j], 0, keepdims=True) for j in range(5)], 0
    )
    for p in range(PIECES):
        comm.pack[p] = pack_ref[p * PIECE : (p + 1) * PIECE]
    comm.swap_halves()
    back = mm(sums, transposed(ew1_ref[D : 2 * D]))
    local_ref[...] += back[0:NODES] + mm(sums_r, transposed(ew1_ref[2 * D : 3 * D]))
    ghost_out_ref[...] = back[NODES:].reshape(FACES, SLOTS, D)
    comm.reduce_in_plane()
    comm.send_ghosts(ghost_out_ref)
    comm.reduce_along_z()
    node_out_ref[...] = comm.add_ghosts(local_ref[...], rows_ref)
    comm.spread()
    out_ref[...] = comm.fin[...]
    comm.drain()


VMEM = pl.BlockSpec(memory_space=pltpu.VMEM)
HBM = pl.BlockSpec(memory_space=pltpu.HBM)
INPUTS = 17


def fused(args, scales):
    scratch = [pltpu.VMEM(a.shape, a.dtype) for a in args]
    scratch += [
        pltpu.SemaphoreType.DMA((INPUTS,)),
        pltpu.VMEM((FULL + NODES + D, D), BF),
        pltpu.VMEM((EDGES, D), BF),
        pltpu.VMEM((EDGES, D), BF),
        pltpu.VMEM((EDGES, D), F32),
        pltpu.VMEM((EDGES, D), F32),
        pltpu.VMEM((EDGES, D), F32),
        pltpu.VMEM((EDGES, D), F32),
        pltpu.VMEM((EDGES, D), BF),
        pltpu.VMEM((EDGES, D), BF),
        pltpu.VMEM((NODES, D), F32),
        pltpu.VMEM((FULL + NODES, D), F32),
        pltpu.VMEM((D, D), BF),
        pltpu.VMEM((D, D), BF),
        pltpu.VMEM((D, D), BF),
        pltpu.VMEM((NODES, D), BF),
        pltpu.VMEM((5, 8, D), F32),
        pltpu.VMEM((NODES, D), F32),
        pltpu.VMEM((FACES, SLOTS, D), F32),
        pltpu.VMEM((ROWS, D), F32),
        pltpu.VMEM((PIECES, PIECE, D), F32),
        pltpu.VMEM((16, PIECE, D), F32),
        pltpu.VMEM((16, PIECE, D), F32),
        pltpu.VMEM((16, PIECE, D), F32),
        pltpu.VMEM((8, PIECE, D), F32),
        pltpu.VMEM((PIECES, PIECE, D), F32),
        pltpu.VMEM((FACES, SLOTS, D), F32),
        pltpu.SemaphoreType.DMA,
        pltpu.SemaphoreType.DMA,
    ]
    for n in (16, 16, 8, 8, 16, 16, 16, 16, FACES, FACES):
        scratch.append(pltpu.SemaphoreType.DMA((n,)))
    return pl.pallas_call(
        functools.partial(fused_kernel, scales),
        out_shape=(
            jax.ShapeDtypeStruct((1, 1, 1, EDGES, D), BF),
            jax.ShapeDtypeStruct((PIECES, PIECE, D), F32),
            jax.ShapeDtypeStruct((NODES, D), F32),
        ),
        in_specs=[HBM] * INPUTS,
        out_specs=(VMEM,) * 3,
        scratch_shapes=scratch,
        compiler_params=pltpu.CompilerParams(collective_id=0, has_side_effects=True, vmem_limit_bytes=52 * 2**20),
        cost_estimate=pl.CostEstimate(flops=6_000_000_000, bytes_accessed=6_000_000, transcendentals=800_000),
    )(*[pltpu.with_memory_space_constraint(a, pltpu.HBM) for a in args])


def unpack_kernel(edge_in, pack_in, node_in, edge_out, node_out, ew1, ewh, nw1, nwh, eb, eg, es, nb, ng, sem):
    moves = (
        (edge_in, edge_out),
        (node_in, node_out.at[0, 0, 0]),
        (pack_in.at[ROW_EW1 : ROW_EW1 + 3 * D], ew1),
        (pack_in.at[ROW_EWH : ROW_EWH + D], ewh.at[0]),
        (pack_in.at[ROW_EWH + D : ROW_EWH + 2 * D], ewh.at[1]),
        (pack_in.at[ROW_NW1 : ROW_NW1 + 2 * D], nw1),
        (pack_in.at[ROW_NWH : ROW_NWH + D], nwh.at[0]),
        (pack_in.at[ROW_NWH + D : ROW_NWH + 2 * D], nwh.at[1]),
    )
    copies = [pltpu.make_async_copy(a, b, sem.at[k]) for k, (a, b) in enumerate(moves)]
    for cp in copies:
        cp.start()
    eb[...] = pack_in[ROW_ESM : ROW_ESM + 3]
    eg[...] = pack_in[ROW_ESM + 3 : ROW_ESM + 4].reshape(D)
    es[...] = pack_in[ROW_ESM + 4 : ROW_ESM + 5].reshape(D)
    nb[...] = pack_in[ROW_NSM : ROW_NSM + 3]
    ng[...] = pack_in[ROW_NSM + 3 : ROW_NSM + 4].reshape(D)
    for cp in copies:
        cp.wait()


def unpack(edge, pack, node):
    shapes = ((1, 1, 1, NODES, D), (3 * D, D), (2, D, D), (2 * D, D), (2, D, D), (3, D), (D,), (D,), (3, D), (D,))
    return pl.pallas_call(
        unpack_kernel,
        out_shape=(jax.ShapeDtypeStruct(edge.shape, BF),) + tuple(jax.ShapeDtypeStruct(s, F32) for s in shapes),
        in_specs=[VMEM] * 3,
        out_specs=(HBM,) * 6 + (VMEM,) * 5,
        scratch_shapes=[pltpu.SemaphoreType.DMA((8,))],
        compiler_params=pltpu.CompilerParams(vmem_limit_bytes=8 * 2**20),
        cost_estimate=pl.CostEstimate(flops=1_000_000, bytes_accessed=4_000_000, transcendentals=0),
    )(edge, pack, node)


def on_device(
    node_latent, ghost_latent, edge_latent, senders, receivers, export_rows, node_cotangent, edge_cotangent,
    w_edge_in, w_edge_hidden, b_edge, gain_edge, shift_edge, w_node_in, w_node_hidden, b_node, gain_node,
):
    devices = lax.axis_size("gx") * lax.axis_size("gy") * lax.axis_size("gz")
    scales = (float(EDGES * devices) ** (-0.5), float(NODES * devices) ** (-0.5))
    edge, summed, node = fused(
        (
            node_latent, ghost_latent, w_edge_in, w_edge_hidden, senders, receivers, edge_latent,
            b_edge, gain_edge, shift_edge, w_node_in, w_node_hidden, b_node, gain_node,
            node_cotangent, edge_cotangent, export_rows.reshape(FACES, 1, SLOTS),
        ),
        scales,
    )
    edge_grad, node_grad, ew1, ewh, nw1, nwh, eb, eg, es, nb, ng = unpack(edge, summed.reshape(ROWS, D), node)
    return (node_grad, edge_grad, ew1, ewh, eb, eg, es, nw1, nwh, nb, ng)


def solution(mesh):
    block = lambda dims: P("gx", "gy", "gz", *([None] * dims))
    in_specs = tuple(block(k) for k in (2, 3, 2, 1, 1, 2, 2, 2)) + (P(),) * 9
    out_specs = (block(2), block(2)) + (P(),) * 9
    return jax.shard_map(on_device, mesh=mesh, in_specs=in_specs, out_specs=out_specs, check_vma=False)
```

```python
import functools

import jax
import jax.numpy as jnp
from jax import lax
from jax.experimental import pallas as pl
from jax.experimental.pallas import tpu as pltpu
from jax.sharding import PartitionSpec as P

EPSILON = 1e-05
MESH = pl.DeviceIdType.MESH
BF = jnp.bfloat16
F32 = jnp.float32
D = 128
NODES = 512
FACES = 6
SLOTS = 64
FULL = NODES + FACES * SLOTS
EDGES = 2816
CH = 1408
CHUNKS = EDGES // CH
SEND_TILES = FULL // D
RECV_TILES = NODES // D
TILES = SEND_TILES + RECV_TILES
PIECES = 32
EDGE_PIECE = 21
NODE_PIECE = 17
EDGE_ROWS = PIECES * EDGE_PIECE
NODE_ROWS = PIECES * NODE_PIECE
ROW_EWH = 3 * D
ROW_ESM = 5 * D
ROW_NWH = 2 * D
ROW_NSM = 4 * D


PLANE_ORDER = (10, 9, 11, 6, 14, 2, 8, 5, 7, 13, 15, 1, 3, 4, 12)
Z_ORDER = (4, 3, 5, 2, 6, 1, 7)


def mm(a, b):
    return jnp.dot(a, b, preferred_element_type=F32)


def mm_tn(a, b):
    return lax.dot_general(a, b, (((0,), (0,)), ((), ())), preferred_element_type=F32)


def transposed(w):
    return w.astype(F32).T.astype(BF)


def silu_parts(p):
    s = 0.5 * jnp.tanh(0.5 * p) + 0.5
    z = p * s
    return z, s + z * (1.0 - s)


def norm_parts(p):
    c = p - jnp.mean(p, -1, keepdims=True)
    inv = lax.rsqrt(jnp.mean(c * c, -1, keepdims=True) + EPSILON)
    return c * inv, inv


def norm_back(u, gain, n, inv):
    t = u * gain
    return inv * (t - jnp.mean(t, -1, keepdims=True) - n * jnp.mean(t * n, -1, keepdims=True))


def fold(x):
    return jnp.sum(x.reshape(x.shape[0] // 8, 8, x.shape[1]), 0)


def row_sum(x):
    return jnp.sum(fold(x), 0, keepdims=True)


def column_digits(ids_row):
    lo, hi = [], []
    for j in range(ids_row.shape[1] // D):
        t = jnp.broadcast_to(ids_row[:, j * D : (j + 1) * D], (D, D)).T
        lo.append((t & (D - 1)).astype(F32).astype(BF))
        hi.append((t >> 7).astype(F32).astype(BF))
    return jnp.concatenate(lo, 0), jnp.concatenate(hi, 0)


def one_hot_columns(lo, hi, tiles):
    lane = lax.broadcasted_iota(jnp.int32, lo.shape, 1).astype(F32).astype(BF)
    zero = jnp.zeros(lo.shape, BF)
    base = jnp.where(lo == lane, jnp.ones(lo.shape, BF), zero)
    return [jnp.where(hi == BF(k), base, zero) for k in range(tiles)]


def one_hot_rows(ids_row, tiles):
    n = ids_row.shape[1]
    lo = jnp.broadcast_to((ids_row & (D - 1)).astype(F32), (D, n)).astype(BF)
    hi = jnp.broadcast_to((ids_row >> 7).astype(F32), (D, n)).astype(BF)
    row = lax.broadcasted_iota(jnp.int32, (D, n), 0).astype(F32).astype(BF)
    zero = jnp.zeros((D, n), BF)
    base = jnp.where(lo == row, jnp.ones((D, n), BF), zero)
    return [jnp.where(hi == BF(k), base, zero) for k in range(tiles)]


class Place:
    def __init__(self):
        gx, gy, gz = lax.axis_index("gx"), lax.axis_index("gy"), lax.axis_index("gz")
        self.y, self.zl = gx // 2, gx % 2
        self.x, self.c = gz // 2, gz % 2
        self.z = gy * 2 + self.zl
        self.at = (gx, gy, gz)
        self.plane = self.x * 4 + self.y
        self.sibling = (gx, gy, gz + 1 - 2 * self.c)
        self.started = []
        self.ghost_to = []
        for f in range(FACES):
            step = 1 if f % 2 == 0 else -1
            self.ghost_to.append((
                ((gx + step + 8) % 8, gy, gz),
                (gx, (gy + step + 4) % 4, gz),
                (gx, gy, (gz + step + 8) % 8),
            )[f // 2])

    def plane_peer(self, d):
        px, py = (self.x + d // 4) % 4, (self.y + d % 4) % 4
        return px * 4 + py, (py * 2 + self.zl, self.at[1], px * 2 + self.c)

    def z_peer(self, d):
        pz = (self.z + d) % 8
        return (self.y * 2 + pz % 2, pz // 2, self.at[2])

    def greet(self):
        barrier = pltpu.get_barrier_semaphore()
        peers = [self.sibling] + [self.plane_peer(d)[1] for d in PLANE_ORDER]
        peers += [self.z_peer(d) for d in Z_ORDER] + self.ghost_to
        for peer in peers:
            pl.semaphore_signal(barrier, inc=1, device_id=peer, device_id_type=MESH)
        self.greeted = len(peers)

    def meet(self):
        pl.semaphore_wait(pltpu.get_barrier_semaphore(), self.greeted)

    def remote(self, src, dst, send, recv, peer):
        cp = pltpu.make_async_remote_copy(
            src_ref=src, dst_ref=dst, send_sem=send, recv_sem=recv, device_id=peer, device_id_type=MESH
        )
        cp.start()
        self.started.append(cp)
        return cp

    def drain(self):
        for cp in self.started:
            cp.wait_send()


class AllReduce:
    def __init__(self, place, piece, refs):
        self.place, self.piece = place, piece
        (
            self.src, self.pair, self.half, self.inbox, self.zbuf, self.fin,
            self.pair_s, self.pair_r, self.rs_s, self.rs_r, self.z_s, self.z_r,
            self.ag_s, self.ag_r, self.back_s, self.back_r,
        ) = refs

    def swap_halves(self, pack_ref):
        for p in range(PIECES):
            self.src[p] = pack_ref[p * self.piece : (p + 1) * self.piece]
        place = self.place
        other = self.src.at[pl.ds((1 - place.c) * 16, 16)]
        self.pending = [place.remote(other, self.pair, self.pair_s.at[0], self.pair_r.at[0], place.sibling)]

    def arrived(self):
        for cp in self.pending:
            cp.wait_recv()

    def in_plane(self):
        place = self.place
        self.arrived()
        self.half[...] = self.src[pl.ds(place.c * 16, 16)] + self.pair[...]
        self.pending = []
        for d in PLANE_ORDER:
            index, peer = place.plane_peer(d)
            self.pending.append(
                place.remote(self.half.at[index], self.inbox.at[d], self.rs_s.at[d], self.rs_r.at[d], peer)
            )

    def along_z(self):
        self.arrived()
        own = self.half[self.place.plane]
        for d in range(1, 16):
            own = own + self.inbox[d]
        z = self.place.z
        self.zbuf[z] = own
        piece = self.zbuf.at[z]
        self.pending = [
            self.place.remote(piece, piece, self.z_s.at[d], self.z_r.at[d], self.place.z_peer(d)) for d in Z_ORDER
        ]

    def spread(self):
        place = self.place
        self.arrived()
        own = self.zbuf[0]
        for d in range(1, 8):
            own = own + self.zbuf[d]
        mine = place.c * 16 + place.plane
        self.fin[mine] = own
        piece = self.fin.at[mine]
        self.pending = [
            place.remote(piece, piece, self.ag_s.at[d], self.ag_r.at[d], place.plane_peer(d)[1]) for d in PLANE_ORDER
        ]
        self.backs = [place.remote(piece, piece, self.back_s.at[0], self.back_r.at[0], place.sibling)]

    def swap_back(self):
        place = self.place
        for d, cp in reversed(list(zip(PLANE_ORDER, self.pending))):
            cp.wait_recv()
            source = (4 - d // 4) % 4 * 4 + (4 - d % 4) % 4
            piece = self.fin.at[place.c * 16 + place.plane_peer(source)[0]]
            self.backs.append(place.remote(piece, piece, self.back_s.at[d], self.back_r.at[d], place.sibling))
        self.pending = self.backs

    def finish(self, out_ref):
        self.arrived()
        for p in range(PIECES):
            out_ref[p * self.piece : (p + 1) * self.piece] = self.fin[p]


def send_ghosts(place, ghost_ref, gbuf, send, recv):
    return [place.remote(ghost_ref.at[f], gbuf.at[f], send.at[f], recv.at[f], place.ghost_to[f]) for f in range(FACES)]


def add_ghosts(total, copies, gbuf, rows_ref):
    for f in range(FACES):
        copies[f].wait_recv()
        got = gbuf[f]
        high = got.astype(BF)
        low = (got - high.astype(F32)).astype(BF)
        ids = jnp.broadcast_to(rows_ref[f], (NODES, SLOTS))
        hot = jnp.where(ids == lax.broadcasted_iota(jnp.int32, (NODES, SLOTS), 0), 1.0, 0.0).astype(BF)
        total = total + (mm(hot, high) + mm(hot, low))
    return total


def fused_kernel(scales, *refs):
    inputs, refs = refs[:INPUTS], refs[INPUTS:]
    edge_out_ref, edge_sum_ref, node_sum_ref, node_out_ref = refs[:4]
    held, refs = refs[4 : 4 + INPUTS], refs[4 + INPUTS :]
    in_sem = refs[0]
    (
        table, z1, z2, sl1, sl2, nrm, inv, rlo, rhi, agg, acc, w3t, w2t, w1t, aggb, small,
        local_ref, ghost_out_ref, pack_ref, node_pack_ref, full_t, g1b,
    ) = refs[1:23]
    edge_comm, node_comm, (gbuf, g_s, g_r) = refs[23:39], refs[39:55], refs[55:]
    loads = [pltpu.make_async_copy(a, b, in_sem.at[k]) for k, (a, b) in enumerate(zip(inputs, held))]
    for cp in loads:
        cp.start()
    place = Place()
    place.greet()
    edge_reduce = AllReduce(place, EDGE_PIECE, edge_comm)
    node_reduce = AllReduce(place, NODE_PIECE, node_comm)
    (
        node_ref, ghost_ref, ew1_ref, ewh_ref, send_ref, recv_ref, edge_ref, eb_ref, eg_ref, es_ref,
        nw1_ref, nwh_ref, nb_ref, ng_ref, ncot_ref, ecot_ref, rows_ref,
    ) = held
    edge_scale, node_scale = scales
    for cp in loads[:4]:
        cp.wait()
    node = node_ref[0, 0, 0]
    ghosts = ghost_ref[0, 0, 0].reshape(FACES * SLOTS, D)
    full = jnp.concatenate([node, ghosts], 0)
    table[0:FULL] = mm(full, ew1_ref[D : 2 * D]).astype(BF)
    table[FULL : FULL + NODES] = mm(node, ew1_ref[2 * D : 3 * D]).astype(BF)
    table[FULL + NODES :] = ew1_ref[0:D]
    w3t[...] = transposed(ewh_ref[1])
    w2t[...] = transposed(ewh_ref[0])
    w1t[...] = transposed(ew1_ref[0:D])
    agg[...] = jnp.zeros_like(agg)
    acc[...] = jnp.zeros_like(acc)
    small[...] = jnp.zeros_like(small)
    pack_ref[...] = jnp.zeros_like(pack_ref)
    node_pack_ref[ROW_NSM:] = jnp.zeros((NODE_ROWS - ROW_NSM, D), F32)
    for cp in loads[4:10]:
        cp.wait()
    egain = eg_ref[...].reshape(1, D)
    eshift = es_ref[...].reshape(1, D)

    def forward(i, carry):
        off = pl.multiple_of(i * CH, CH)
        rows = pl.ds(off, CH)
        s_row = send_ref[0, 0, :, rows]
        r_row = recv_ref[0, 0, :, rows]
        slo, shi = column_digits(s_row)
        lo, hi = column_digits(r_row)
        rlo[rows] = lo
        rhi[rows] = hi
        hot = one_hot_columns(slo, shi, SEND_TILES) + one_hot_columns(lo, hi, RECV_TILES)
        lhs = jnp.concatenate(hot + [edge_ref[0, 0, 0, rows]], 1)
        p1 = mm(lhs, table[...]) + eb_ref[0:1]
        a1, d1 = silu_parts(p1)
        b1 = a1.astype(BF)
        z1[rows] = b1
        sl1[rows] = d1
        p2 = mm(b1, ewh_ref[0]) + eb_ref[1:2]
        a2, d2 = silu_parts(p2)
        b2 = a2.astype(BF)
        z2[rows] = b2
        sl2[rows] = d2
        q = mm(b2, ewh_ref[1]) + eb_ref[2:3]
        n, iv = norm_parts(q)
        nrm[rows] = n
        inv[rows] = jnp.broadcast_to(iv, (CH, D))
        new = (n * egain + eshift).astype(BF)
        hot_t = jnp.concatenate(one_hot_rows(r_row, RECV_TILES), 0)
        agg[...] += mm(hot_t, new)
        return carry

    lax.fori_loop(0, CHUNKS, forward, 0)

    for cp in loads[10:]:
        cp.wait()
    ngain = ng_ref[...].reshape(1, D)
    node_in = jnp.concatenate([node, agg[...].astype(BF)], 1)
    a1, d1 = silu_parts(mm(node_in, nw1_ref[...]) + nb_ref[0:1])
    b1 = a1.astype(BF)
    a2, d2 = silu_parts(mm(b1, nwh_ref[0]) + nb_ref[1:2])
    b2 = a2.astype(BF)
    n, iv = norm_parts(mm(b2, nwh_ref[1]) + nb_ref[2:3])
    u = ncot_ref[0, 0, 0].astype(F32)
    g3 = norm_back(u, ngain, n, iv)
    h3 = g3.astype(BF)
    g2 = mm(h3, transposed(nwh_ref[1])) * d2
    h2 = g2.astype(BF)
    g1 = mm(h2, transposed(nwh_ref[0])) * d1
    h1 = g1.astype(BF)
    local_ref[...] = u + mm(h1, transposed(nw1_ref[0:D]))
    aggb[...] = mm(h1, transposed(nw1_ref[D : 2 * D])).astype(BF)
    node_pack_ref[0 : 2 * D] = mm_tn(node_in, h1) * node_scale
    node_pack_ref[ROW_NWH : ROW_NWH + D] = mm_tn(b1, h2) * node_scale
    node_pack_ref[ROW_NWH + D : ROW_NWH + 2 * D] = mm_tn(b2, h3) * node_scale
    node_pack_ref[ROW_NSM : ROW_NSM + 4] = node_scale * jnp.concatenate(
        [row_sum(g1), row_sum(g2), row_sum(g3), row_sum(u * n)], 0
    )
    full_t[...] = full.astype(F32).T.astype(BF)
    place.meet()
    node_reduce.swap_halves(node_pack_ref)

    def backward(i, carry):
        rows = pl.ds(i * CH, CH)
        s_row = send_ref[0, 0, :, rows]
        r_row = recv_ref[0, 0, :, rows]
        hot = jnp.concatenate(one_hot_columns(rlo[rows], rhi[rows], RECV_TILES), 1)
        cot = ecot_ref[0, 0, 0, rows].astype(F32)
        u = cot + mm(hot, aggb[...])
        n = nrm[rows]
        g3 = norm_back(u, egain, n, inv[rows])
        h3 = g3.astype(BF)
        g2 = mm(h3, w3t[...]) * sl2[rows]
        h2 = g2.astype(BF)
        g1 = mm(h2, w2t[...]) * sl1[rows]
        h1 = g1.astype(BF)
        g1b[rows] = h1
        pack_ref[0:D] += mm_tn(edge_ref[0, 0, 0, rows], h1)
        pack_ref[ROW_EWH : ROW_EWH + D] += mm_tn(z1[rows], h2)
        pack_ref[ROW_EWH + D : ROW_EWH + 2 * D] += mm_tn(z2[rows], h3)
        hot_t = jnp.concatenate(one_hot_rows(s_row, SEND_TILES) + one_hot_rows(r_row, RECV_TILES), 0)
        acc[...] += mm(hot_t, h1)
        small[0] += fold(g1)
        small[1] += fold(g2)
        small[2] += fold(g3)
        small[3] += fold(u * n)
        small[4] += fold(u)
        return carry

    for i in range(CHUNKS):
        backward(i, 0)
        if i == 0:
            node_reduce.in_plane()

    sums = acc[0:FULL].astype(BF)
    sums_r = acc[FULL : FULL + NODES].astype(BF)
    pack_ref[0:D] = pack_ref[0:D] * edge_scale
    pack_ref[D : 2 * D] = mm(full_t[...], sums) * edge_scale
    pack_ref[2 * D : 3 * D] = mm(full_t[:, 0:NODES], sums_r) * edge_scale
    pack_ref[ROW_EWH : ROW_EWH + 2 * D] = pack_ref[ROW_EWH : ROW_EWH + 2 * D] * edge_scale
    pack_ref[ROW_ESM : ROW_ESM + 5] = edge_scale * jnp.concatenate(
        [jnp.sum(small[j], 0, keepdims=True) for j in range(5)], 0
    )
    edge_reduce.swap_halves(pack_ref)
    back = mm(sums, transposed(ew1_ref[D : 2 * D]))
    ghost_out_ref[...] = back[NODES:].reshape(FACES, SLOTS, D)
    node_reduce.along_z()
    edge_reduce.in_plane()
    ghosts = send_ghosts(place, ghost_out_ref, gbuf, g_s, g_r)
    local_ref[...] += back[0:NODES] + mm(sums_r, transposed(ew1_ref[2 * D : 3 * D]))
    edge_out_ref[0, 0, 0] = (ecot_ref[0, 0, 0].astype(F32) + mm(g1b[...], w1t[...])).astype(BF)
    node_reduce.spread()
    edge_reduce.along_z()
    node_out_ref[...] = add_ghosts(local_ref[...], ghosts, gbuf, rows_ref)
    edge_reduce.spread()
    node_reduce.swap_back()
    edge_reduce.swap_back()
    node_reduce.finish(node_sum_ref)
    edge_reduce.finish(edge_sum_ref)
    place.drain()


VMEM = pl.BlockSpec(memory_space=pltpu.VMEM)
HBM = pl.BlockSpec(memory_space=pltpu.HBM)
INPUTS = 17


def fused(args, scales):
    scratch = [pltpu.VMEM(a.shape, a.dtype) for a in args]
    scratch += [
        pltpu.SemaphoreType.DMA((INPUTS,)),
        pltpu.VMEM((FULL + NODES + D, D), BF),
        pltpu.VMEM((EDGES, D), BF),
        pltpu.VMEM((EDGES, D), BF),
        pltpu.VMEM((EDGES, D), F32),
        pltpu.VMEM((EDGES, D), F32),
        pltpu.VMEM((EDGES, D), F32),
        pltpu.VMEM((EDGES, D), F32),
        pltpu.VMEM((EDGES, D), BF),
        pltpu.VMEM((EDGES, D), BF),
        pltpu.VMEM((NODES, D), F32),
        pltpu.VMEM((FULL + NODES, D), F32),
        pltpu.VMEM((D, D), BF),
        pltpu.VMEM((D, D), BF),
        pltpu.VMEM((D, D), BF),
        pltpu.VMEM((NODES, D), BF),
        pltpu.VMEM((5, 8, D), F32),
        pltpu.VMEM((NODES, D), F32),
        pltpu.VMEM((FACES, SLOTS, D), F32),
        pltpu.VMEM((EDGE_ROWS, D), F32),
        pltpu.VMEM((NODE_ROWS, D), F32),
        pltpu.VMEM((D, FULL), BF),
        pltpu.VMEM((EDGES, D), BF),
    ]
    for piece in (EDGE_PIECE, NODE_PIECE):
        scratch += [pltpu.VMEM((n, piece, D), F32) for n in (PIECES, 16, 16, 16, 8, PIECES)]
        scratch += [pltpu.SemaphoreType.DMA((n,)) for n in (1, 1, 16, 16, 8, 8, 16, 16, 16, 16)]
    scratch += [
        pltpu.VMEM((FACES, SLOTS, D), F32),
        pltpu.SemaphoreType.DMA((FACES,)),
        pltpu.SemaphoreType.DMA((FACES,)),
    ]
    return pl.pallas_call(
        functools.partial(fused_kernel, scales),
        out_shape=(
            jax.ShapeDtypeStruct((1, 1, 1, EDGES, D), BF),
            jax.ShapeDtypeStruct((EDGE_ROWS, D), F32),
            jax.ShapeDtypeStruct((NODE_ROWS, D), F32),
            jax.ShapeDtypeStruct((NODES, D), F32),
        ),
        in_specs=[HBM] * INPUTS,
        out_specs=(VMEM,) * 4,
        scratch_shapes=scratch,
        compiler_params=pltpu.CompilerParams(collective_id=0, has_side_effects=True, vmem_limit_bytes=52 * 2**20),
        cost_estimate=pl.CostEstimate(flops=6_000_000_000, bytes_accessed=6_000_000, transcendentals=800_000),
    )(*[pltpu.with_memory_space_constraint(a, pltpu.HBM) for a in args])


def unpack_kernel(
    edge_in, edge_sum, node_sum, node_in,
    edge_out, node_out, ew1, ewh, nw1, nwh, eb, eg, es, nb, ng,
    eb_v, eg_v, es_v, nb_v, ng_v, sem,
):
    eb_v[...] = edge_sum[ROW_ESM : ROW_ESM + 3]
    eg_v[...] = edge_sum[ROW_ESM + 3 : ROW_ESM + 4].reshape(D)
    es_v[...] = edge_sum[ROW_ESM + 4 : ROW_ESM + 5].reshape(D)
    nb_v[...] = node_sum[ROW_NSM : ROW_NSM + 3]
    ng_v[...] = node_sum[ROW_NSM + 3 : ROW_NSM + 4].reshape(D)
    moves = (
        (edge_in, edge_out),
        (node_in, node_out.at[0, 0, 0]),
        (edge_sum.at[0 : 3 * D], ew1),
        (edge_sum.at[ROW_EWH : ROW_EWH + D], ewh.at[0]),
        (edge_sum.at[ROW_EWH + D : ROW_EWH + 2 * D], ewh.at[1]),
        (node_sum.at[0 : 2 * D], nw1),
        (node_sum.at[ROW_NWH : ROW_NWH + D], nwh.at[0]),
        (node_sum.at[ROW_NWH + D : ROW_NWH + 2 * D], nwh.at[1]),
        (eb_v, eb),
        (eg_v, eg),
        (es_v, es),
        (nb_v, nb),
        (ng_v, ng),
    )
    copies = [pltpu.make_async_copy(a, b, sem.at[k]) for k, (a, b) in enumerate(moves)]
    for cp in copies:
        cp.start()
    for cp in copies:
        cp.wait()


def unpack(edge, edge_sum, node_sum, node):
    shapes = ((1, 1, 1, NODES, D), (3 * D, D), (2, D, D), (2 * D, D), (2, D, D), (3, D), (D,), (D,), (3, D), (D,))
    return pl.pallas_call(
        unpack_kernel,
        out_shape=(jax.ShapeDtypeStruct(edge.shape, BF),) + tuple(jax.ShapeDtypeStruct(s, F32) for s in shapes),
        in_specs=[VMEM] * 4,
        out_specs=(HBM,) * 11,
        scratch_shapes=[pltpu.VMEM(s, F32) for s in shapes[5:]] + [pltpu.SemaphoreType.DMA((13,))],
        compiler_params=pltpu.CompilerParams(vmem_limit_bytes=8 * 2**20),
        cost_estimate=pl.CostEstimate(flops=1_000_000, bytes_accessed=4_000_000, transcendentals=0),
    )(edge, edge_sum, node_sum, node)


def on_device(
    node_latent, ghost_latent, edge_latent, senders, receivers, export_rows, node_cotangent, edge_cotangent,
    w_edge_in, w_edge_hidden, b_edge, gain_edge, shift_edge, w_node_in, w_node_hidden, b_node, gain_node,
):
    devices = lax.axis_size("gx") * lax.axis_size("gy") * lax.axis_size("gz")
    scales = (float(EDGES * devices) ** (-0.5), float(NODES * devices) ** (-0.5))
    edge, edge_sum, node_sum, node = fused(
        (
            node_latent, ghost_latent, w_edge_in, w_edge_hidden, senders, receivers, edge_latent,
            b_edge, gain_edge, shift_edge, w_node_in, w_node_hidden, b_node, gain_node,
            node_cotangent, edge_cotangent, export_rows.reshape(FACES, 1, SLOTS),
        ),
        scales,
    )
    edge_grad, node_grad, ew1, ewh, nw1, nwh, eb, eg, es, nb, ng = unpack(edge, edge_sum, node_sum, node)
    return (node_grad, edge_grad, ew1, ewh, eb, eg, es, nw1, nwh, nb, ng)


def solution(mesh):
    block = lambda dims: P("gx", "gy", "gz", *([None] * dims))
    in_specs = tuple(block(k) for k in (2, 3, 2, 1, 1, 2, 2, 2)) + (P(),) * 9
    out_specs = (block(2), block(2)) + (P(),) * 9
    return jax.shard_map(on_device, mesh=mesh, in_specs=in_specs, out_specs=out_specs, check_vma=False)
```

```python
import functools

import jax
import jax.numpy as jnp
from jax import lax
from jax.experimental import pallas as pl
from jax.experimental.pallas import tpu as pltpu
from jax.sharding import PartitionSpec as P

EPSILON = 1e-05
MESH = pl.DeviceIdType.MESH
BF = jnp.bfloat16
F32 = jnp.float32
D = 128
NODES = 512
FACES = 6
SLOTS = 64
FULL = NODES + FACES * SLOTS
EDGES = 2816
CH = 1408
CHUNKS = EDGES // CH
SEND_TILES = FULL // D
RECV_TILES = NODES // D
TILES = SEND_TILES + RECV_TILES
PIECES = 32
EDGE_PIECE = 21
NODE_PIECE = 17
EDGE_ROWS = PIECES * EDGE_PIECE
NODE_ROWS = PIECES * NODE_PIECE
ROW_EWH = 3 * D
ROW_ESM = 5 * D
ROW_NWH = 2 * D
ROW_NSM = 4 * D


PLANE_ORDER = (10, 9, 11, 6, 14, 2, 8, 5, 7, 13, 15, 1, 3, 4, 12)
Z_ORDER = (4, 3, 5, 2, 6, 1, 7)


def mm(a, b):
    return jnp.dot(a, b, preferred_element_type=F32)


def mm_tn(a, b):
    return lax.dot_general(a, b, (((0,), (0,)), ((), ())), preferred_element_type=F32)


def mm_nt(a, b):
    return lax.dot_general(a, b, (((1,), (1,)), ((), ())), preferred_element_type=F32)


def transposed(w):
    return w.astype(F32).T.astype(BF)


def silu_parts(p):
    s = 0.5 * jnp.tanh(0.5 * p) + 0.5
    z = p * s
    return z, s + z * (1.0 - s)


def norm_parts(p):
    c = p - jnp.mean(p, 0, keepdims=True)
    inv = lax.rsqrt(jnp.mean(c * c, 0, keepdims=True) + EPSILON)
    return c * inv, inv


def norm_back(u, gain, n, inv):
    t = u * gain
    return inv * (t - jnp.mean(t, 0, keepdims=True) - n * jnp.mean(t * n, 0, keepdims=True))


def wide(column, n):
    return jnp.concatenate([column] * (n // D), 1)


def fold(x):
    total = x[:, 0:D]
    for k in range(1, x.shape[1] // D):
        total = total + x[:, k * D : (k + 1) * D]
    return total


def lane_sum(x):
    return jnp.sum(x.T, 0, keepdims=True)


def column_digits(s_row, r_row):
    both = s_row + (r_row << 10)
    parts = []
    for j in range(both.shape[1] // D):
        t = jnp.broadcast_to(both[:, j * D : (j + 1) * D], (D, D)).T
        digits = (t & (D - 1), (t >> 7) & 7, (t >> 10) & (D - 1), t >> 17)
        parts.append([d.astype(F32).astype(BF) for d in digits])
    return [jnp.concatenate(p, 0) for p in zip(*parts)]


def one_hot_columns(lo, hi, tiles):
    lane = lax.broadcasted_iota(jnp.int32, lo.shape, 1).astype(F32).astype(BF)
    zero = jnp.zeros(lo.shape, BF)
    base = jnp.where(lo == lane, jnp.ones(lo.shape, BF), zero)
    return [jnp.where(hi == BF(k), base, zero) for k in range(tiles)]


def one_hot_rows(ids_row, tiles):
    n = ids_row.shape[1]
    lo = jnp.broadcast_to((ids_row & (D - 1)).astype(F32), (D, n)).astype(BF)
    hi = jnp.broadcast_to((ids_row >> 7).astype(F32), (D, n)).astype(BF)
    row = lax.broadcasted_iota(jnp.int32, (D, n), 0).astype(F32).astype(BF)
    zero = jnp.zeros((D, n), BF)
    base = jnp.where(lo == row, jnp.ones((D, n), BF), zero)
    return [jnp.where(hi == BF(k), base, zero) for k in range(tiles)]


class Place:
    def __init__(self):
        gx, gy, gz = lax.axis_index("gx"), lax.axis_index("gy"), lax.axis_index("gz")
        self.y, self.zl = gx // 2, gx % 2
        self.x, self.c = gz // 2, gz % 2
        self.z = gy * 2 + self.zl
        self.at = (gx, gy, gz)
        self.plane = self.x * 4 + self.y
        self.sibling = (gx, gy, gz + 1 - 2 * self.c)
        self.started = []
        self.ghost_to = []
        for f in range(FACES):
            step = 1 if f % 2 == 0 else -1
            self.ghost_to.append((
                ((gx + step + 8) % 8, gy, gz),
                (gx, (gy + step + 4) % 4, gz),
                (gx, gy, (gz + step + 8) % 8),
            )[f // 2])

    def plane_peer(self, d):
        px, py = (self.x + d // 4) % 4, (self.y + d % 4) % 4
        return px * 4 + py, (py * 2 + self.zl, self.at[1], px * 2 + self.c)

    def z_peer(self, d):
        pz = (self.z + d) % 8
        return (self.y * 2 + pz % 2, pz // 2, self.at[2])

    def greet(self):
        barrier = pltpu.get_barrier_semaphore()
        peers = [self.sibling] + [self.plane_peer(d)[1] for d in PLANE_ORDER]
        peers += [self.z_peer(d) for d in Z_ORDER] + self.ghost_to
        for peer in peers:
            pl.semaphore_signal(barrier, inc=1, device_id=peer, device_id_type=MESH)
        self.greeted = len(peers)

    def meet(self):
        pl.semaphore_wait(pltpu.get_barrier_semaphore(), self.greeted)

    def remote(self, src, dst, send, recv, peer):
        cp = pltpu.make_async_remote_copy(
            src_ref=src, dst_ref=dst, send_sem=send, recv_sem=recv, device_id=peer, device_id_type=MESH
        )
        cp.start()
        self.started.append(cp)
        return cp

    def drain(self):
        for cp in self.started:
            cp.wait_send()


class AllReduce:
    def __init__(self, place, piece, refs):
        self.place, self.piece = place, piece
        (
            self.src, self.pair, self.half, self.inbox, self.zbuf, self.fin,
            self.pair_s, self.pair_r, self.rs_s, self.rs_r, self.z_s, self.z_r,
            self.ag_s, self.ag_r, self.back_s, self.back_r,
        ) = refs

    def swap_halves(self, pack_ref):
        for p in range(PIECES):
            self.src[p] = pack_ref[p * self.piece : (p + 1) * self.piece]
        place = self.place
        other = self.src.at[pl.ds((1 - place.c) * 16, 16)]
        self.pending = [place.remote(other, self.pair, self.pair_s.at[0], self.pair_r.at[0], place.sibling)]

    def arrived(self):
        for cp in self.pending:
            cp.wait_recv()

    def in_plane(self):
        place = self.place
        self.arrived()
        self.half[...] = self.src[pl.ds(place.c * 16, 16)] + self.pair[...]
        self.pending = []
        for d in PLANE_ORDER:
            index, peer = place.plane_peer(d)
            self.pending.append(
                place.remote(self.half.at[index], self.inbox.at[d], self.rs_s.at[d], self.rs_r.at[d], peer)
            )

    def along_z(self):
        self.arrived()
        own = self.half[self.place.plane]
        for d in range(1, 16):
            own = own + self.inbox[d]
        z = self.place.z
        self.zbuf[z] = own
        piece = self.zbuf.at[z]
        self.pending = [
            self.place.remote(piece, piece, self.z_s.at[d], self.z_r.at[d], self.place.z_peer(d)) for d in Z_ORDER
        ]

    def spread(self):
        place = self.place
        self.arrived()
        own = self.zbuf[0]
        for d in range(1, 8):
            own = own + self.zbuf[d]
        mine = place.c * 16 + place.plane
        self.fin[mine] = own
        piece = self.fin.at[mine]
        self.pending = [
            place.remote(piece, piece, self.ag_s.at[d], self.ag_r.at[d], place.plane_peer(d)[1]) for d in PLANE_ORDER
        ]
        self.backs = [place.remote(piece, piece, self.back_s.at[0], self.back_r.at[0], place.sibling)]

    def swap_back(self):
        place = self.place
        for d, cp in reversed(list(zip(PLANE_ORDER, self.pending))):
            cp.wait_recv()
            source = (4 - d // 4) % 4 * 4 + (4 - d % 4) % 4
            piece = self.fin.at[place.c * 16 + place.plane_peer(source)[0]]
            self.backs.append(place.remote(piece, piece, self.back_s.at[d], self.back_r.at[d], place.sibling))
        self.pending = self.backs

    def finish(self, out_ref):
        self.arrived()
        for p in range(PIECES):
            out_ref[p * self.piece : (p + 1) * self.piece] = self.fin[p]


def send_ghosts(place, ghost_ref, gbuf, send, recv):
    return [place.remote(ghost_ref.at[f], gbuf.at[f], send.at[f], recv.at[f], place.ghost_to[f]) for f in range(FACES)]


def add_ghosts(total, copies, gbuf, rows_ref):
    for f in range(FACES):
        copies[f].wait_recv()
        got = gbuf[f]
        high = got.astype(BF)
        low = (got - high.astype(F32)).astype(BF)
        ids = jnp.broadcast_to(rows_ref[f], (NODES, SLOTS))
        hot = jnp.where(ids == lax.broadcasted_iota(jnp.int32, (NODES, SLOTS), 0), 1.0, 0.0).astype(BF)
        total = total + (mm(hot, high) + mm(hot, low))
    return total


def fused_kernel(scales, *refs):
    inputs, refs = refs[:INPUTS], refs[INPUTS:]
    edge_out_ref, edge_sum_ref, node_sum_ref, node_out_ref = refs[:4]
    held, refs = refs[4 : 4 + INPUTS], refs[4 + INPUTS :]
    in_sem = refs[0]
    (
        table_t, full_t, z1, z2, sl1, sl2, nrm, inv, slo, shi, rlo, rhi, g1b, agg, acc, aggb, small, cols,
        w2t, w3t, node_h1, local_ref, ghost_out_ref, pack_ref, node_pack_ref,
    ) = refs[1:26]
    edge_comm, node_comm, (gbuf, g_s, g_r) = refs[26:42], refs[42:58], refs[58:]
    loads = [pltpu.make_async_copy(a, b, in_sem.at[k]) for k, (a, b) in enumerate(zip(inputs, held))]
    for cp in loads:
        cp.start()
    place = Place()
    place.greet()
    edge_reduce = AllReduce(place, EDGE_PIECE, edge_comm)
    node_reduce = AllReduce(place, NODE_PIECE, node_comm)
    (
        node_ref, ghost_ref, ew1_ref, ewh_ref, send_ref, recv_ref, edge_ref, eb_ref, eg_ref, es_ref,
        nw1_ref, nwh_ref, nb_ref, ng_ref, ncot_ref, ecot_ref, rows_ref,
    ) = held
    edge_scale, node_scale = scales
    for cp in loads[:4]:
        cp.wait()
    ghosts = ghost_ref[0, 0, 0].reshape(FACES * SLOTS, D)
    full_t[...] = jnp.concatenate([transposed(node_ref[0, 0, 0]), transposed(ghosts)], 1)
    table_t[:, 0:FULL] = mm(transposed(ew1_ref[D : 2 * D]), full_t[...]).astype(BF)
    table_t[:, FULL : FULL + NODES] = mm(transposed(ew1_ref[2 * D : 3 * D]), full_t[:, 0:NODES]).astype(BF)
    table_t[:, FULL + NODES :] = transposed(ew1_ref[0:D])
    w2t[...] = transposed(ewh_ref[0])
    w3t[...] = transposed(ewh_ref[1])
    node_pack_ref[ROW_NSM:] = jnp.zeros((NODE_ROWS - ROW_NSM, D), F32)
    pack_ref[ROW_ESM:] = jnp.zeros((EDGE_ROWS - ROW_ESM, D), F32)
    for cp in loads[4:14]:
        cp.wait()
    columns = [eb_ref[k : k + 1] for k in range(3)] + [eg_ref[...].reshape(1, D), es_ref[...].reshape(1, D)]
    columns += [nb_ref[k : k + 1] for k in range(3)] + [ng_ref[...].reshape(1, D)]
    for k, column in enumerate(columns):
        cols[k] = jnp.broadcast_to(column, (D, D)).T

    def forward(i, carry):
        off = pl.multiple_of(i * CH, CH)
        at = pl.ds(off, CH)
        s_row = send_ref[0, 0, :, at]
        r_row = recv_ref[0, 0, :, at]
        hot = one_hot_rows(s_row, SEND_TILES) + one_hot_rows(r_row, RECV_TILES)
        rhs = jnp.concatenate(hot + [transposed(edge_ref[0, 0, 0, at])], 0)
        p1 = mm(table_t[...], rhs) + wide(cols[0], CH)
        a1, d1 = silu_parts(p1)
        b1 = a1.astype(BF)
        z1[i] = b1
        sl1[i] = d1
        p2 = mm(w2t[...], b1) + wide(cols[1], CH)
        a2, d2 = silu_parts(p2)
        b2 = a2.astype(BF)
        z2[i] = b2
        sl2[i] = d2
        q = mm(w3t[...], b2) + wide(cols[2], CH)
        n, iv = norm_parts(q)
        nrm[i] = n
        inv[i] = iv
        new = (n * wide(cols[3], CH) + wide(cols[4], CH)).astype(BF)
        slo[at], shi[at], lo, hi = column_digits(s_row, r_row)
        rlo[at], rhi[at] = lo, hi
        part = mm(new, jnp.concatenate(one_hot_columns(lo, hi, RECV_TILES), 1))

        @pl.when(i == 0)
        def _():
            agg[...] = part

        @pl.when(i > 0)
        def _():
            agg[...] += part

        return carry

    lax.fori_loop(0, CHUNKS, forward, 0)

    for cp in loads[14:]:
        cp.wait()
    node_in = jnp.concatenate([full_t[:, 0:NODES], agg[...].astype(BF)], 0)
    a1, d1 = silu_parts(mm(transposed(nw1_ref[...]), node_in) + wide(cols[5], NODES))
    b1 = a1.astype(BF)
    a2, d2 = silu_parts(mm(transposed(nwh_ref[0]), b1) + wide(cols[6], NODES))
    b2 = a2.astype(BF)
    n, iv = norm_parts(mm(transposed(nwh_ref[1]), b2) + wide(cols[7], NODES))
    u = transposed(ncot_ref[0, 0, 0]).astype(F32)
    g3 = norm_back(u, wide(cols[8], NODES), n, iv)
    h3 = g3.astype(BF)
    g2 = mm(nwh_ref[1], h3) * d2
    h2 = g2.astype(BF)
    g1 = mm(nwh_ref[0], h2) * d1
    h1 = g1.astype(BF)
    node_h1[...] = h1
    aggb[...] = mm(nw1_ref[D : 2 * D], h1).astype(BF)
    node_pack_ref[0 : 2 * D] = mm_nt(node_in, h1) * node_scale
    node_pack_ref[ROW_NWH : ROW_NWH + D] = mm_nt(b1, h2) * node_scale
    node_pack_ref[ROW_NWH + D : ROW_NWH + 2 * D] = mm_nt(b2, h3) * node_scale
    node_pack_ref[ROW_NSM : ROW_NSM + 4] = node_scale * jnp.concatenate(
        [lane_sum(fold(g1)), lane_sum(fold(g2)), lane_sum(fold(g3)), lane_sum(fold(u * n))], 0
    )
    place.meet()
    node_reduce.swap_halves(node_pack_ref)

    def backward(i):
        at = pl.ds(i * CH, CH)
        first = i == 0

        def add(ref, where, value):
            if first:
                ref[where] = value
            else:
                ref[where] += value

        r_row = recv_ref[0, 0, :, at]
        cot = transposed(ecot_ref[0, 0, 0, at]).astype(F32)
        u = cot + mm(aggb[...], jnp.concatenate(one_hot_rows(r_row, RECV_TILES), 0))
        n = nrm[i]
        g3 = norm_back(u, wide(cols[3], CH), n, inv[i])
        h3 = g3.astype(BF)
        g2 = mm(ewh_ref[1], h3) * sl2[i]
        h2 = g2.astype(BF)
        g1 = mm(ewh_ref[0], h2) * sl1[i]
        h1 = g1.astype(BF)
        g1b[i] = h1
        add(pack_ref, pl.ds(ROW_EWH, D), mm_nt(z1[i], h2))
        add(pack_ref, pl.ds(ROW_EWH + D, D), mm_nt(z2[i], h3))
        hot = one_hot_columns(slo[at], shi[at], SEND_TILES) + one_hot_columns(rlo[at], rhi[at], RECV_TILES)
        add(acc, slice(None), mm(h1, jnp.concatenate(hot + [edge_ref[0, 0, 0, at]], 1)))
        for k, x in enumerate((g1, g2, g3, u * n, u)):
            add(small, k, fold(x))

    for i in range(CHUNKS):
        backward(i)
        if i == 0:
            node_reduce.in_plane()

    sums = acc[:, 0:FULL].astype(BF)
    sums_r = acc[:, FULL : FULL + NODES].astype(BF)
    pack_ref[0:D] = acc[:, FULL + NODES :].T * edge_scale
    pack_ref[D : 2 * D] = mm_nt(full_t[...], sums) * edge_scale
    pack_ref[2 * D : 3 * D] = mm_nt(full_t[:, 0:NODES], sums_r) * edge_scale
    pack_ref[ROW_EWH : ROW_EWH + 2 * D] = pack_ref[ROW_EWH : ROW_EWH + 2 * D] * edge_scale
    pack_ref[ROW_ESM : ROW_ESM + 5] = edge_scale * jnp.concatenate([lane_sum(small[j]) for j in range(5)], 0)
    edge_reduce.swap_halves(pack_ref)
    back = mm_tn(sums, transposed(ew1_ref[D : 2 * D]))
    ghost_out_ref[...] = back[NODES:].reshape(FACES, SLOTS, D)
    node_reduce.along_z()
    edge_reduce.in_plane()
    ghosts = send_ghosts(place, ghost_out_ref, gbuf, g_s, g_r)
    local_ref[...] = (
        ncot_ref[0, 0, 0].astype(F32)
        + mm_tn(node_h1[...], transposed(nw1_ref[0:D]))
        + back[0:NODES]
        + mm_tn(sums_r, transposed(ew1_ref[2 * D : 3 * D]))
    )
    for i in range(CHUNKS):
        at = pl.ds(i * CH, CH)
        edge_out_ref[0, 0, 0, at] = (
            ecot_ref[0, 0, 0, at].astype(F32) + mm_tn(g1b[i], transposed(ew1_ref[0:D]))
        ).astype(BF)
    node_reduce.spread()
    edge_reduce.along_z()
    node_out_ref[...] = add_ghosts(local_ref[...], ghosts, gbuf, rows_ref)
    edge_reduce.spread()
    node_reduce.swap_back()
    edge_reduce.swap_back()
    node_reduce.finish(node_sum_ref)
    edge_reduce.finish(edge_sum_ref)
    place.drain()


VMEM = pl.BlockSpec(memory_space=pltpu.VMEM)
HBM = pl.BlockSpec(memory_space=pltpu.HBM)
INPUTS = 17


def fused(args, scales):
    scratch = [pltpu.VMEM(a.shape, a.dtype) for a in args]
    scratch += [
        pltpu.SemaphoreType.DMA((INPUTS,)),
        pltpu.VMEM((D, FULL + NODES + D), BF),
        pltpu.VMEM((D, FULL), BF),
        pltpu.VMEM((CHUNKS, D, CH), BF),
        pltpu.VMEM((CHUNKS, D, CH), BF),
        pltpu.VMEM((CHUNKS, D, CH), F32),
        pltpu.VMEM((CHUNKS, D, CH), F32),
        pltpu.VMEM((CHUNKS, D, CH), F32),
        pltpu.VMEM((CHUNKS, 1, CH), F32),
        pltpu.VMEM((EDGES, D), BF),
        pltpu.VMEM((EDGES, D), BF),
        pltpu.VMEM((EDGES, D), BF),
        pltpu.VMEM((EDGES, D), BF),
        pltpu.VMEM((CHUNKS, D, CH), BF),
        pltpu.VMEM((D, NODES), F32),
        pltpu.VMEM((D, FULL + NODES + D), F32),
        pltpu.VMEM((D, NODES), BF),
        pltpu.VMEM((5, D, D), F32),
        pltpu.VMEM((9, D, D), F32),
        pltpu.VMEM((D, D), BF),
        pltpu.VMEM((D, D), BF),
        pltpu.VMEM((D, NODES), BF),
        pltpu.VMEM((NODES, D), F32),
        pltpu.VMEM((FACES, SLOTS, D), F32),
        pltpu.VMEM((EDGE_ROWS, D), F32),
        pltpu.VMEM((NODE_ROWS, D), F32),
    ]
    for piece in (EDGE_PIECE, NODE_PIECE):
        scratch += [pltpu.VMEM((n, piece, D), F32) for n in (PIECES, 16, 16, 16, 8, PIECES)]
        scratch += [pltpu.SemaphoreType.DMA((n,)) for n in (1, 1, 16, 16, 8, 8, 16, 16, 16, 16)]
    scratch += [
        pltpu.VMEM((FACES, SLOTS, D), F32),
        pltpu.SemaphoreType.DMA((FACES,)),
        pltpu.SemaphoreType.DMA((FACES,)),
    ]
    return pl.pallas_call(
        functools.partial(fused_kernel, scales),
        out_shape=(
            jax.ShapeDtypeStruct((1, 1, 1, EDGES, D), BF),
            jax.ShapeDtypeStruct((EDGE_ROWS, D), F32),
            jax.ShapeDtypeStruct((NODE_ROWS, D), F32),
            jax.ShapeDtypeStruct((NODES, D), F32),
        ),
        in_specs=[HBM] * INPUTS,
        out_specs=(VMEM,) * 4,
        scratch_shapes=scratch,
        compiler_params=pltpu.CompilerParams(collective_id=0, has_side_effects=True, vmem_limit_bytes=52 * 2**20),
        cost_estimate=pl.CostEstimate(flops=6_000_000_000, bytes_accessed=6_000_000, transcendentals=800_000),
    )(*[pltpu.with_memory_space_constraint(a, pltpu.HBM) for a in args])


def unpack_kernel(
    edge_in, edge_sum, node_sum, node_in,
    edge_out, node_out, ew1, ewh, nw1, nwh, eb, eg, es, nb, ng,
    eb_v, eg_v, es_v, nb_v, ng_v, sem,
):
    eb_v[...] = edge_sum[ROW_ESM : ROW_ESM + 3]
    eg_v[...] = edge_sum[ROW_ESM + 3 : ROW_ESM + 4].reshape(D)
    es_v[...] = edge_sum[ROW_ESM + 4 : ROW_ESM + 5].reshape(D)
    nb_v[...] = node_sum[ROW_NSM : ROW_NSM + 3]
    ng_v[...] = node_sum[ROW_NSM + 3 : ROW_NSM + 4].reshape(D)
    moves = (
        (edge_in, edge_out),
        (node_in, node_out.at[0, 0, 0]),
        (edge_sum.at[0 : 3 * D], ew1),
        (edge_sum.at[ROW_EWH : ROW_EWH + D], ewh.at[0]),
        (edge_sum.at[ROW_EWH + D : ROW_EWH + 2 * D], ewh.at[1]),
        (node_sum.at[0 : 2 * D], nw1),
        (node_sum.at[ROW_NWH : ROW_NWH + D], nwh.at[0]),
        (node_sum.at[ROW_NWH + D : ROW_NWH + 2 * D], nwh.at[1]),
        (eb_v, eb),
        (eg_v, eg),
        (es_v, es),
        (nb_v, nb),
        (ng_v, ng),
    )
    copies = [pltpu.make_async_copy(a, b, sem.at[k]) for k, (a, b) in enumerate(moves)]
    for cp in copies:
        cp.start()
    for cp in copies:
        cp.wait()


def unpack(edge, edge_sum, node_sum, node):
    shapes = ((1, 1, 1, NODES, D), (3 * D, D), (2, D, D), (2 * D, D), (2, D, D), (3, D), (D,), (D,), (3, D), (D,))
    return pl.pallas_call(
        unpack_kernel,
        out_shape=(jax.ShapeDtypeStruct(edge.shape, BF),) + tuple(jax.ShapeDtypeStruct(s, F32) for s in shapes),
        in_specs=[VMEM] * 4,
        out_specs=(HBM,) * 11,
        scratch_shapes=[pltpu.VMEM(s, F32) for s in shapes[5:]] + [pltpu.SemaphoreType.DMA((13,))],
        compiler_params=pltpu.CompilerParams(vmem_limit_bytes=8 * 2**20),
        cost_estimate=pl.CostEstimate(flops=1_000_000, bytes_accessed=4_000_000, transcendentals=0),
    )(edge, edge_sum, node_sum, node)


def on_device(
    node_latent, ghost_latent, edge_latent, senders, receivers, export_rows, node_cotangent, edge_cotangent,
    w_edge_in, w_edge_hidden, b_edge, gain_edge, shift_edge, w_node_in, w_node_hidden, b_node, gain_node,
):
    devices = lax.axis_size("gx") * lax.axis_size("gy") * lax.axis_size("gz")
    scales = (float(EDGES * devices) ** (-0.5), float(NODES * devices) ** (-0.5))
    edge, edge_sum, node_sum, node = fused(
        (
            node_latent, ghost_latent, w_edge_in, w_edge_hidden, senders, receivers, edge_latent,
            b_edge, gain_edge, shift_edge, w_node_in, w_node_hidden, b_node, gain_node,
            node_cotangent, edge_cotangent, export_rows.reshape(FACES, 1, SLOTS),
        ),
        scales,
    )
    edge_grad, node_grad, ew1, ewh, nw1, nwh, eb, eg, es, nb, ng = unpack(edge, edge_sum, node_sum, node)
    return (node_grad, edge_grad, ew1, ewh, eb, eg, es, nw1, nwh, nb, ng)


def solution(mesh):
    block = lambda dims: P("gx", "gy", "gz", *([None] * dims))
    in_specs = tuple(block(k) for k in (2, 3, 2, 1, 1, 2, 2, 2)) + (P(),) * 9
    out_specs = (block(2), block(2)) + (P(),) * 9
    return jax.shard_map(on_device, mesh=mesh, in_specs=in_specs, out_specs=out_specs, check_vma=False)
```

```python
import functools

import jax
import jax.numpy as jnp
from jax import lax
from jax.experimental import pallas as pl
from jax.experimental.pallas import tpu as pltpu
from jax.sharding import PartitionSpec as P

EPSILON = 1e-05
MESH = pl.DeviceIdType.MESH
BF = jnp.bfloat16
F32 = jnp.float32
D = 128
NODES = 512
FACES = 6
SLOTS = 64
FULL = NODES + FACES * SLOTS
EDGES = 2816
CH = 1408
CHUNKS = EDGES // CH
SEND_TILES = FULL // D
RECV_TILES = NODES // D
TILES = SEND_TILES + RECV_TILES
PIECES = 32
EDGE_PIECE = 21
NODE_PIECE = 17
EDGE_ROWS = PIECES * EDGE_PIECE
NODE_ROWS = PIECES * NODE_PIECE
ROW_EWH = 3 * D
ROW_ESM = 5 * D
ROW_NWH = 2 * D
ROW_NSM = 4 * D


PLANE_ORDER = (10, 9, 11, 6, 14, 2, 8, 5, 7, 13, 15, 1, 3, 4, 12)
Z_ORDER = (4, 3, 5, 2, 6, 1, 7)


def mm(a, b):
    return jnp.dot(a, b, preferred_element_type=F32)


def mm_tn(a, b):
    return lax.dot_general(a, b, (((0,), (0,)), ((), ())), preferred_element_type=F32)


def mm_nt(a, b):
    return lax.dot_general(a, b, (((1,), (1,)), ((), ())), preferred_element_type=F32)


def transposed(w):
    return w.T


def halved(w):
    return (w.astype(F32) * 0.5).astype(BF)


def silu_parts(h):
    t = jnp.tanh(h)
    z = h + h * t
    return z, (1.0 + t) + z * (1.0 - t)


def norm_parts(p):
    c = p - jnp.mean(p, 0, keepdims=True)
    inv = lax.rsqrt(jnp.mean(c * c, 0, keepdims=True) + EPSILON)
    return c * inv, inv


def norm_back(u, gain, n, inv):
    t = u * gain
    return inv * (t - jnp.mean(t, 0, keepdims=True) - n * jnp.mean(t * n, 0, keepdims=True))


def wide(column, n):
    return jnp.concatenate([column] * (n // D), 1)


def fold(x):
    total = x[:, 0:D]
    for k in range(1, x.shape[1] // D):
        total = total + x[:, k * D : (k + 1) * D]
    return total


def lane_sum(x):
    return jnp.sum(x.T, 0, keepdims=True)


def column_digits(ids_row):
    parts = []
    for digit in (ids_row & (D - 1), ids_row >> 7):
        row = digit.astype(F32)
        tiles = [
            jnp.broadcast_to(row[:, j : j + D], (D, D)).astype(BF).T for j in range(0, ids_row.shape[1], D)
        ]
        parts.append(jnp.concatenate(tiles, 0))
    return parts


def one_hot_columns(lo, hi, tiles):
    lane = lax.broadcasted_iota(jnp.int32, lo.shape, 1).astype(F32).astype(BF)
    zero = jnp.zeros(lo.shape, BF)
    base = jnp.where(lo == lane, jnp.ones(lo.shape, BF), zero)
    return [jnp.where(hi == BF(k), base, zero) for k in range(tiles)]


def one_hot_rows(ids_row, tiles):
    n = ids_row.shape[1]
    lo = jnp.broadcast_to((ids_row & (D - 1)).astype(F32), (D, n)).astype(BF)
    hi = jnp.broadcast_to((ids_row >> 7).astype(F32), (D, n)).astype(BF)
    row = lax.broadcasted_iota(jnp.int32, (D, n), 0).astype(F32).astype(BF)
    zero = jnp.zeros((D, n), BF)
    base = jnp.where(lo == row, jnp.ones((D, n), BF), zero)
    return [jnp.where(hi == BF(k), base, zero) for k in range(tiles)]


class Place:
    def __init__(self):
        gx, gy, gz = lax.axis_index("gx"), lax.axis_index("gy"), lax.axis_index("gz")
        self.y, self.zl = gx // 2, gx % 2
        self.x, self.c = gz // 2, gz % 2
        self.z = gy * 2 + self.zl
        self.at = (gx, gy, gz)
        self.plane = self.x * 4 + self.y
        self.sibling = (gx, gy, gz + 1 - 2 * self.c)
        self.started = []
        self.ghost_to = []
        for f in range(FACES):
            step = 1 if f % 2 == 0 else -1
            self.ghost_to.append((
                ((gx + step + 8) % 8, gy, gz),
                (gx, (gy + step + 4) % 4, gz),
                (gx, gy, (gz + step + 8) % 8),
            )[f // 2])

    def plane_peer(self, d):
        px, py = (self.x + d // 4) % 4, (self.y + d % 4) % 4
        return px * 4 + py, (py * 2 + self.zl, self.at[1], px * 2 + self.c)

    def z_peer(self, d):
        pz = (self.z + d) % 8
        return (self.y * 2 + pz % 2, pz // 2, self.at[2])

    def greet(self):
        barrier = pltpu.get_barrier_semaphore()
        peers = [self.sibling] + [self.plane_peer(d)[1] for d in PLANE_ORDER]
        peers += [self.z_peer(d) for d in Z_ORDER] + self.ghost_to
        for peer in peers:
            pl.semaphore_signal(barrier, inc=1, device_id=peer, device_id_type=MESH)
        self.greeted = len(peers)

    def meet(self):
        pl.semaphore_wait(pltpu.get_barrier_semaphore(), self.greeted)

    def remote(self, src, dst, send, recv, peer):
        cp = pltpu.make_async_remote_copy(
            src_ref=src, dst_ref=dst, send_sem=send, recv_sem=recv, device_id=peer, device_id_type=MESH
        )
        cp.start()
        self.started.append(cp)
        return cp

    def drain(self):
        for cp in self.started:
            cp.wait_send()


class AllReduce:
    def __init__(self, place, piece, refs):
        self.place, self.piece = place, piece
        (
            self.src, self.pair, self.half, self.inbox, self.zbuf, self.fin,
            self.pair_s, self.pair_r, self.rs_s, self.rs_r, self.z_s, self.z_r,
            self.ag_s, self.ag_r, self.back_s, self.back_r,
        ) = refs

    def swap_halves(self, pack_ref):
        for p in range(PIECES):
            self.src[p] = pack_ref[p * self.piece : (p + 1) * self.piece]
        place = self.place
        other = self.src.at[pl.ds((1 - place.c) * 16, 16)]
        self.pending = [place.remote(other, self.pair, self.pair_s.at[0], self.pair_r.at[0], place.sibling)]

    def arrived(self):
        for cp in self.pending:
            cp.wait_recv()

    def in_plane(self):
        place = self.place
        self.arrived()
        self.half[...] = self.src[pl.ds(place.c * 16, 16)] + self.pair[...]
        self.pending = []
        for d in PLANE_ORDER:
            index, peer = place.plane_peer(d)
            self.pending.append(
                place.remote(self.half.at[index], self.inbox.at[d], self.rs_s.at[d], self.rs_r.at[d], peer)
            )

    def along_z(self):
        self.arrived()
        own = self.half[self.place.plane]
        for d in range(1, 16):
            own = own + self.inbox[d]
        z = self.place.z
        self.zbuf[z] = own
        piece = self.zbuf.at[z]
        self.pending = [
            self.place.remote(piece, piece, self.z_s.at[d], self.z_r.at[d], self.place.z_peer(d)) for d in Z_ORDER
        ]

    def spread(self):
        place = self.place
        self.arrived()
        own = self.zbuf[0]
        for d in range(1, 8):
            own = own + self.zbuf[d]
        mine = place.c * 16 + place.plane
        self.fin[mine] = own
        piece = self.fin.at[mine]
        self.pending = [
            place.remote(piece, piece, self.ag_s.at[d], self.ag_r.at[d], place.plane_peer(d)[1]) for d in PLANE_ORDER
        ]
        self.backs = [place.remote(piece, piece, self.back_s.at[0], self.back_r.at[0], place.sibling)]

    def swap_back(self):
        place = self.place
        for d, cp in reversed(list(zip(PLANE_ORDER, self.pending))):
            cp.wait_recv()
            source = (4 - d // 4) % 4 * 4 + (4 - d % 4) % 4
            piece = self.fin.at[place.c * 16 + place.plane_peer(source)[0]]
            self.backs.append(place.remote(piece, piece, self.back_s.at[d], self.back_r.at[d], place.sibling))
        self.pending = self.backs

    def finish(self, out_ref):
        self.arrived()
        for p in range(PIECES):
            out_ref[p * self.piece : (p + 1) * self.piece] = self.fin[p]


def send_ghosts(place, ghost_ref, gbuf, send, recv):
    return [place.remote(ghost_ref.at[f], gbuf.at[f], send.at[f], recv.at[f], place.ghost_to[f]) for f in range(FACES)]


def add_ghosts(total, copies, gbuf, rows_ref):
    for f in range(FACES):
        copies[f].wait_recv()
        got = gbuf[f]
        high = got.astype(BF)
        low = (got - high.astype(F32)).astype(BF)
        ids = jnp.broadcast_to(rows_ref[f], (NODES, SLOTS))
        hot = jnp.where(ids == lax.broadcasted_iota(jnp.int32, (NODES, SLOTS), 0), 1.0, 0.0).astype(BF)
        total = total + (mm(hot, high) + mm(hot, low))
    return total


def fused_kernel(scales, *refs):
    inputs, refs = refs[:INPUTS], refs[INPUTS:]
    edge_out_ref, edge_sum_ref, node_sum_ref, node_out_ref = refs[:4]
    held, refs = refs[4 : 4 + INPUTS], refs[4 + INPUTS :]
    in_sem = refs[0]
    (
        table_t, full_t, z1, z2, sl1, sl2, nrm, inv, slo, shi, to_rows, to_cols, g1b, agg, acc, aggb, small, cols,
        w2t, w3t, w2h, w3h, node_h1, local_ref, ghost_out_ref, pack_ref, node_pack_ref,
    ) = refs[1:28]
    edge_comm, node_comm, (gbuf, g_s, g_r) = refs[28:44], refs[44:60], refs[60:]
    loads = [pltpu.make_async_copy(a, b, in_sem.at[k]) for k, (a, b) in enumerate(zip(inputs, held))]
    for cp in loads:
        cp.start()
    place = Place()
    place.greet()
    edge_reduce = AllReduce(place, EDGE_PIECE, edge_comm)
    node_reduce = AllReduce(place, NODE_PIECE, node_comm)
    (
        node_ref, ghost_ref, ew1_ref, ewh_ref, send_ref, recv_ref, edge_ref, eb_ref, eg_ref, es_ref,
        nw1_ref, nwh_ref, nb_ref, ng_ref, ncot_ref, ecot_ref, rows_ref,
    ) = held
    edge_scale, node_scale = scales
    for cp in loads[:4]:
        cp.wait()
    ghosts = ghost_ref[0, 0, 0].reshape(FACES * SLOTS, D)
    full_t[...] = jnp.concatenate([transposed(node_ref[0, 0, 0]), transposed(ghosts)], 1)
    table_t[:, 0:FULL] = mm(halved(transposed(ew1_ref[D : 2 * D])), full_t[...]).astype(BF)
    table_t[:, FULL + NODES :] = halved(transposed(ew1_ref[0:D]))
    w2t[...] = halved(transposed(ewh_ref[0]))
    w3t[...] = transposed(ewh_ref[1])
    w2h[...] = halved(ewh_ref[0])
    w3h[...] = halved(ewh_ref[1])
    node_pack_ref[ROW_NSM:] = jnp.zeros((NODE_ROWS - ROW_NSM, D), F32)
    pack_ref[ROW_ESM:] = jnp.zeros((EDGE_ROWS - ROW_ESM, D), F32)
    for cp in loads[4:14]:
        cp.wait()
    columns = [eb_ref[k : k + 1] for k in range(3)] + [eg_ref[...].reshape(1, D), es_ref[...].reshape(1, D)]
    columns += [nb_ref[k : k + 1] for k in range(3)] + [ng_ref[...].reshape(1, D)]
    halves = (0, 1, 5, 6)
    for k, column in enumerate(columns):
        cols[k] = jnp.broadcast_to(column * 0.5 if k in halves else column, (D, D)).T
    table_t[:, FULL : FULL + NODES] = (
        mm(halved(transposed(ew1_ref[2 * D : 3 * D])), full_t[:, 0:NODES]) + wide(cols[0], NODES)
    ).astype(BF)

    def forward(i, carry):
        off = pl.multiple_of(i * CH, CH)
        at = pl.ds(off, CH)
        s_row = send_ref[0, 0, :, at]
        r_row = recv_ref[0, 0, :, at]
        to = jnp.concatenate(one_hot_rows(r_row, RECV_TILES), 0)
        to_rows[i] = to
        rhs = jnp.concatenate(one_hot_rows(s_row, SEND_TILES) + [to, transposed(edge_ref[0, 0, 0, at])], 0)
        p1 = mm(table_t[...], rhs)
        a1, d1 = silu_parts(p1)
        b1 = a1.astype(BF)
        z1[i] = b1
        sl1[i] = d1
        p2 = mm(w2t[...], b1) + wide(cols[1], CH)
        a2, d2 = silu_parts(p2)
        b2 = a2.astype(BF)
        z2[i] = b2
        sl2[i] = d2
        q = mm(w3t[...], b2) + wide(cols[2], CH)
        n, iv = norm_parts(q)
        nrm[i] = n
        inv[i] = iv
        new = (n * wide(cols[3], CH) + wide(cols[4], CH)).astype(BF)
        slo[at], shi[at] = column_digits(s_row)
        to = jnp.concatenate(one_hot_columns(*column_digits(r_row), RECV_TILES), 1)
        to_cols[at] = to
        part = mm(new, to)

        @pl.when(i == 0)
        def _():
            agg[...] = part

        @pl.when(i > 0)
        def _():
            agg[...] += part

        return carry

    lax.fori_loop(0, CHUNKS, forward, 0)

    for cp in loads[14:]:
        cp.wait()
    node_in = jnp.concatenate([full_t[:, 0:NODES], agg[...].astype(BF)], 0)
    a1, d1 = silu_parts(mm(halved(transposed(nw1_ref[...])), node_in) + wide(cols[5], NODES))
    b1 = a1.astype(BF)
    a2, d2 = silu_parts(mm(halved(transposed(nwh_ref[0])), b1) + wide(cols[6], NODES))
    b2 = a2.astype(BF)
    n, iv = norm_parts(mm(transposed(nwh_ref[1]), b2) + wide(cols[7], NODES))
    u = transposed(ncot_ref[0, 0, 0]).astype(F32)
    g3 = norm_back(u, wide(cols[8], NODES), n, iv)
    h3 = g3.astype(BF)
    g2 = mm(halved(nwh_ref[1]), h3) * d2
    h2 = g2.astype(BF)
    g1 = mm(halved(nwh_ref[0]), h2) * d1
    h1 = g1.astype(BF)
    node_h1[...] = h1
    aggb[...] = mm(nw1_ref[D : 2 * D], h1).astype(BF)
    node_pack_ref[0 : 2 * D] = mm_nt(node_in, h1) * node_scale
    node_pack_ref[ROW_NWH : ROW_NWH + D] = mm_nt(b1, h2) * node_scale
    node_pack_ref[ROW_NWH + D : ROW_NWH + 2 * D] = mm_nt(b2, h3) * node_scale
    node_pack_ref[ROW_NSM : ROW_NSM + 4] = node_scale * jnp.concatenate(
        [lane_sum(fold(g1)), lane_sum(fold(g2)), lane_sum(fold(g3)), lane_sum(fold(u * n))], 0
    )
    place.meet()
    node_reduce.swap_halves(node_pack_ref)

    def backward(i):
        at = pl.ds(i * CH, CH)
        first = i == 0

        def add(ref, where, value):
            if first:
                ref[where] = value
            else:
                ref[where] += value

        cot = transposed(ecot_ref[0, 0, 0, at]).astype(F32)
        u = cot + mm(aggb[...], to_rows[i])
        n = nrm[i]
        g3 = norm_back(u, wide(cols[3], CH), n, inv[i])
        h3 = g3.astype(BF)
        g2 = mm(w3h[...], h3) * sl2[i]
        h2 = g2.astype(BF)
        g1 = mm(w2h[...], h2) * sl1[i]
        h1 = g1.astype(BF)
        g1b[i] = h1
        ones = jnp.ones((16, CH), BF)
        for k, (z, h) in enumerate(((z1[i], h2), (z2[i], h3))):
            grad = mm_nt(jnp.concatenate([z, ones], 0), h)
            add(pack_ref, pl.ds(ROW_EWH + k * D, D), grad[0:D])
            add(pack_ref, pl.ds(ROW_ESM + 1 + k, 1), grad[D : D + 1])
        hot = one_hot_columns(slo[at], shi[at], SEND_TILES)
        add(acc, slice(None), mm(h1, jnp.concatenate(hot + [to_cols[at], edge_ref[0, 0, 0, at]], 1)))
        for k, x in enumerate((u * n, u)):
            add(small, k, fold(x))

    for i in range(CHUNKS):
        backward(i)
        if i == 0:
            node_reduce.in_plane()

    sums = acc[:, 0:FULL].astype(BF)
    sums_r = acc[:, FULL : FULL + NODES].astype(BF)
    pack_ref[0:D] = acc[:, FULL + NODES :].T * edge_scale
    pack_ref[D : 2 * D] = mm_nt(full_t[...], sums) * edge_scale
    pack_ref[2 * D : 3 * D] = mm_nt(full_t[:, 0:NODES], sums_r) * edge_scale
    pack_ref[ROW_EWH : ROW_EWH + 2 * D] = pack_ref[ROW_EWH : ROW_EWH + 2 * D] * edge_scale
    pack_ref[ROW_ESM + 1 : ROW_ESM + 3] = pack_ref[ROW_ESM + 1 : ROW_ESM + 3] * edge_scale
    pack_ref[ROW_ESM : ROW_ESM + 1] = lane_sum(fold(acc[:, FULL : FULL + NODES])) * edge_scale
    pack_ref[ROW_ESM + 3 : ROW_ESM + 5] = edge_scale * jnp.concatenate([lane_sum(small[0]), lane_sum(small[1])], 0)
    edge_reduce.swap_halves(pack_ref)
    back = mm_tn(sums, transposed(ew1_ref[D : 2 * D]))
    ghost_out_ref[...] = back[NODES:].reshape(FACES, SLOTS, D)
    edge_reduce.in_plane()
    ghosts = send_ghosts(place, ghost_out_ref, gbuf, g_s, g_r)
    local_ref[...] = (
        ncot_ref[0, 0, 0].astype(F32)
        + mm_tn(node_h1[...], transposed(nw1_ref[0:D]))
        + back[0:NODES]
        + mm_tn(sums_r, transposed(ew1_ref[2 * D : 3 * D]))
    )
    for i in range(CHUNKS):
        at = pl.ds(i * CH, CH)
        edge_out_ref[0, 0, 0, at] = (
            ecot_ref[0, 0, 0, at].astype(F32) + mm_tn(g1b[i], transposed(ew1_ref[0:D]))
        ).astype(BF)
    node_reduce.along_z()
    edge_reduce.along_z()
    node_out_ref[...] = add_ghosts(local_ref[...], ghosts, gbuf, rows_ref)
    node_reduce.spread()
    edge_reduce.spread()
    node_reduce.swap_back()
    edge_reduce.swap_back()
    node_reduce.finish(node_sum_ref)
    edge_reduce.finish(edge_sum_ref)
    place.drain()


VMEM = pl.BlockSpec(memory_space=pltpu.VMEM)
HBM = pl.BlockSpec(memory_space=pltpu.HBM)
INPUTS = 17


def fused(args, scales):
    scratch = [pltpu.VMEM(a.shape, a.dtype) for a in args]
    scratch += [
        pltpu.SemaphoreType.DMA((INPUTS,)),
        pltpu.VMEM((D, FULL + NODES + D), BF),
        pltpu.VMEM((D, FULL), BF),
        pltpu.VMEM((CHUNKS, D, CH), BF),
        pltpu.VMEM((CHUNKS, D, CH), BF),
        pltpu.VMEM((CHUNKS, D, CH), F32),
        pltpu.VMEM((CHUNKS, D, CH), F32),
        pltpu.VMEM((CHUNKS, D, CH), F32),
        pltpu.VMEM((CHUNKS, 1, CH), F32),
        pltpu.VMEM((EDGES, D), BF),
        pltpu.VMEM((EDGES, D), BF),
        pltpu.VMEM((CHUNKS, NODES, CH), BF),
        pltpu.VMEM((EDGES, NODES), BF),
        pltpu.VMEM((CHUNKS, D, CH), BF),
        pltpu.VMEM((D, NODES), F32),
        pltpu.VMEM((D, FULL + NODES + D), F32),
        pltpu.VMEM((D, NODES), BF),
        pltpu.VMEM((2, D, D), F32),
        pltpu.VMEM((9, D, D), F32),
        pltpu.VMEM((D, D), BF),
        pltpu.VMEM((D, D), BF),
        pltpu.VMEM((D, D), BF),
        pltpu.VMEM((D, D), BF),
        pltpu.VMEM((D, NODES), BF),
        pltpu.VMEM((NODES, D), F32),
        pltpu.VMEM((FACES, SLOTS, D), F32),
        pltpu.VMEM((EDGE_ROWS, D), F32),
        pltpu.VMEM((NODE_ROWS, D), F32),
    ]
    for piece in (EDGE_PIECE, NODE_PIECE):
        scratch += [pltpu.VMEM((n, piece, D), F32) for n in (PIECES, 16, 16, 16, 8, PIECES)]
        scratch += [pltpu.SemaphoreType.DMA((n,)) for n in (1, 1, 16, 16, 8, 8, 16, 16, 16, 16)]
    scratch += [
        pltpu.VMEM((FACES, SLOTS, D), F32),
        pltpu.SemaphoreType.DMA((FACES,)),
        pltpu.SemaphoreType.DMA((FACES,)),
    ]
    return pl.pallas_call(
        functools.partial(fused_kernel, scales),
        out_shape=(
            jax.ShapeDtypeStruct((1, 1, 1, EDGES, D), BF),
            jax.ShapeDtypeStruct((EDGE_ROWS, D), F32),
            jax.ShapeDtypeStruct((NODE_ROWS, D), F32),
            jax.ShapeDtypeStruct((NODES, D), F32),
        ),
        in_specs=[HBM] * INPUTS,
        out_specs=(VMEM,) * 4,
        scratch_shapes=scratch,
        compiler_params=pltpu.CompilerParams(collective_id=0, has_side_effects=True, vmem_limit_bytes=52 * 2**20),
        cost_estimate=pl.CostEstimate(flops=6_000_000_000, bytes_accessed=6_000_000, transcendentals=800_000),
    )(*[pltpu.with_memory_space_constraint(a, pltpu.HBM) for a in args])


def unpack_kernel(
    edge_in, edge_sum, node_sum, node_in,
    edge_out, node_out, ew1, ewh, nw1, nwh, eb, eg, es, nb, ng,
    eb_v, eg_v, es_v, nb_v, ng_v, sem,
):
    eb_v[...] = edge_sum[ROW_ESM : ROW_ESM + 3]
    eg_v[...] = edge_sum[ROW_ESM + 3 : ROW_ESM + 4].reshape(D)
    es_v[...] = edge_sum[ROW_ESM + 4 : ROW_ESM + 5].reshape(D)
    nb_v[...] = node_sum[ROW_NSM : ROW_NSM + 3]
    ng_v[...] = node_sum[ROW_NSM + 3 : ROW_NSM + 4].reshape(D)
    moves = (
        (edge_in, edge_out),
        (node_in, node_out.at[0, 0, 0]),
        (edge_sum.at[0 : 3 * D], ew1),
        (edge_sum.at[ROW_EWH : ROW_EWH + D], ewh.at[0]),
        (edge_sum.at[ROW_EWH + D : ROW_EWH + 2 * D], ewh.at[1]),
        (node_sum.at[0 : 2 * D], nw1),
        (node_sum.at[ROW_NWH : ROW_NWH + D], nwh.at[0]),
        (node_sum.at[ROW_NWH + D : ROW_NWH + 2 * D], nwh.at[1]),
        (eb_v, eb),
        (eg_v, eg),
        (es_v, es),
        (nb_v, nb),
        (ng_v, ng),
    )
    copies = [pltpu.make_async_copy(a, b, sem.at[k]) for k, (a, b) in enumerate(moves)]
    for cp in copies:
        cp.start()
    for cp in copies:
        cp.wait()


def unpack(edge, edge_sum, node_sum, node):
    shapes = ((1, 1, 1, NODES, D), (3 * D, D), (2, D, D), (2 * D, D), (2, D, D), (3, D), (D,), (D,), (3, D), (D,))
    return pl.pallas_call(
        unpack_kernel,
        out_shape=(jax.ShapeDtypeStruct(edge.shape, BF),) + tuple(jax.ShapeDtypeStruct(s, F32) for s in shapes),
        in_specs=[VMEM] * 4,
        out_specs=(HBM,) * 11,
        scratch_shapes=[pltpu.VMEM(s, F32) for s in shapes[5:]] + [pltpu.SemaphoreType.DMA((13,))],
        compiler_params=pltpu.CompilerParams(vmem_limit_bytes=8 * 2**20),
        cost_estimate=pl.CostEstimate(flops=1_000_000, bytes_accessed=4_000_000, transcendentals=0),
    )(edge, edge_sum, node_sum, node)


def on_device(
    node_latent, ghost_latent, edge_latent, senders, receivers, export_rows, node_cotangent, edge_cotangent,
    w_edge_in, w_edge_hidden, b_edge, gain_edge, shift_edge, w_node_in, w_node_hidden, b_node, gain_node,
):
    devices = lax.axis_size("gx") * lax.axis_size("gy") * lax.axis_size("gz")
    scales = (float(EDGES * devices) ** (-0.5), float(NODES * devices) ** (-0.5))
    edge, edge_sum, node_sum, node = fused(
        (
            node_latent, ghost_latent, w_edge_in, w_edge_hidden, senders, receivers, edge_latent,
            b_edge, gain_edge, shift_edge, w_node_in, w_node_hidden, b_node, gain_node,
            node_cotangent, edge_cotangent, export_rows.reshape(FACES, 1, SLOTS),
        ),
        scales,
    )
    edge_grad, node_grad, ew1, ewh, nw1, nwh, eb, eg, es, nb, ng = unpack(edge, edge_sum, node_sum, node)
    return (node_grad, edge_grad, ew1, ewh, eb, eg, es, nw1, nwh, nb, ng)


def solution(mesh):
    block = lambda dims: P("gx", "gy", "gz", *([None] * dims))
    in_specs = tuple(block(k) for k in (2, 3, 2, 1, 1, 2, 2, 2)) + (P(),) * 9
    out_specs = (block(2), block(2)) + (P(),) * 9
    return jax.shard_map(on_device, mesh=mesh, in_specs=in_specs, out_specs=out_specs, check_vma=False)
```

```python
import functools

import jax
import jax.numpy as jnp
from jax import lax
from jax.experimental import pallas as pl
from jax.experimental.pallas import tpu as pltpu
from jax.sharding import PartitionSpec as P

EPSILON = 1e-05
MESH = pl.DeviceIdType.MESH
BF = jnp.bfloat16
F32 = jnp.float32
D = 128
NODES = 512
FACES = 6
SLOTS = 64
FULL = NODES + FACES * SLOTS
EDGES = 2816
CH = 2816
CHUNKS = EDGES // CH
SEND_TILES = FULL // D
RECV_TILES = NODES // D
TILES = SEND_TILES + RECV_TILES
PIECES = 32
EDGE_PIECE = 21
NODE_PIECE = 17
EDGE_ROWS = PIECES * EDGE_PIECE
NODE_ROWS = PIECES * NODE_PIECE
ROW_EWH = 3 * D
ROW_ESM = 5 * D
ROW_NWH = 2 * D
ROW_NSM = 4 * D


PLANE_ORDER = (10, 9, 11, 6, 14, 2, 8, 5, 7, 13, 15, 1, 3, 4, 12)
Z_ORDER = (4, 3, 5, 2, 6, 1, 7)


def mm(a, b):
    return jnp.dot(a, b, preferred_element_type=F32)


def mm_tn(a, b):
    return lax.dot_general(a, b, (((0,), (0,)), ((), ())), preferred_element_type=F32)


def mm_nt(a, b):
    return lax.dot_general(a, b, (((1,), (1,)), ((), ())), preferred_element_type=F32)


def transposed(w):
    return w.T


def halved(w):
    return (w.astype(F32) * 0.5).astype(BF)


def silu_parts(h):
    t = jnp.tanh(h)
    z = h + h * t
    return z, (1.0 + t) + z * (1.0 - t)


def norm_parts(p):
    c = p - jnp.mean(p, 0, keepdims=True)
    inv = lax.rsqrt(jnp.mean(c * c, 0, keepdims=True) + EPSILON)
    return c * inv, inv


def norm_back(u, gain, n, inv):
    t = u * gain
    return inv * (t - jnp.mean(t, 0, keepdims=True) - n * jnp.mean(t * n, 0, keepdims=True))


def wide(column, n):
    return jnp.concatenate([column] * (n // D), 1)


def fold(x):
    total = x[:, 0:D]
    for k in range(1, x.shape[1] // D):
        total = total + x[:, k * D : (k + 1) * D]
    return total


def lane_sum(x):
    return jnp.sum(x.T, 0, keepdims=True)


def column_digits(ids_row):
    parts = []
    for digit in (ids_row & (D - 1), ids_row >> 7):
        row = digit.astype(F32)
        tiles = [
            jnp.broadcast_to(row[:, j : j + D], (D, D)).astype(BF).T for j in range(0, ids_row.shape[1], D)
        ]
        parts.append(jnp.concatenate(tiles, 0))
    return parts


def one_hot_columns(lo, hi, tiles):
    lane = lax.broadcasted_iota(jnp.int32, lo.shape, 1).astype(F32).astype(BF)
    zero = jnp.zeros(lo.shape, BF)
    base = jnp.where(lo == lane, jnp.ones(lo.shape, BF), zero)
    return [jnp.where(hi == BF(k), base, zero) for k in range(tiles)]


def one_hot_rows(ids_row, tiles):
    n = ids_row.shape[1]
    lo = jnp.broadcast_to((ids_row & (D - 1)).astype(F32), (D, n)).astype(BF)
    hi = jnp.broadcast_to((ids_row >> 7).astype(F32), (D, n)).astype(BF)
    row = lax.broadcasted_iota(jnp.int32, (D, n), 0).astype(F32).astype(BF)
    zero = jnp.zeros((D, n), BF)
    base = jnp.where(lo == row, jnp.ones((D, n), BF), zero)
    return [jnp.where(hi == BF(k), base, zero) for k in range(tiles)]


class Place:
    def __init__(self):
        gx, gy, gz = lax.axis_index("gx"), lax.axis_index("gy"), lax.axis_index("gz")
        self.y, self.zl = gx // 2, gx % 2
        self.x, self.c = gz // 2, gz % 2
        self.z = gy * 2 + self.zl
        self.at = (gx, gy, gz)
        self.plane = self.x * 4 + self.y
        self.sibling = (gx, gy, gz + 1 - 2 * self.c)
        self.started = []
        self.ghost_to = []
        for f in range(FACES):
            step = 1 if f % 2 == 0 else -1
            self.ghost_to.append((
                ((gx + step + 8) % 8, gy, gz),
                (gx, (gy + step + 4) % 4, gz),
                (gx, gy, (gz + step + 8) % 8),
            )[f // 2])

    def plane_peer(self, d):
        px, py = (self.x + d // 4) % 4, (self.y + d % 4) % 4
        return px * 4 + py, (py * 2 + self.zl, self.at[1], px * 2 + self.c)

    def z_peer(self, d):
        pz = (self.z + d) % 8
        return (self.y * 2 + pz % 2, pz // 2, self.at[2])

    def greet(self):
        barrier = pltpu.get_barrier_semaphore()
        peers = [self.sibling] + [self.plane_peer(d)[1] for d in PLANE_ORDER]
        peers += [self.z_peer(d) for d in Z_ORDER] + self.ghost_to
        for peer in peers:
            pl.semaphore_signal(barrier, inc=1, device_id=peer, device_id_type=MESH)
        self.greeted = len(peers)

    def meet(self):
        pl.semaphore_wait(pltpu.get_barrier_semaphore(), self.greeted)

    def remote(self, src, dst, send, recv, peer):
        cp = pltpu.make_async_remote_copy(
            src_ref=src, dst_ref=dst, send_sem=send, recv_sem=recv, device_id=peer, device_id_type=MESH
        )
        cp.start()
        self.started.append(cp)
        return cp

    def drain(self, count):
        for cp in self.started[:count]:
            cp.wait_send()
        self.started = self.started[count:]


class AllReduce:
    def __init__(self, place, piece, refs):
        self.place, self.piece = place, piece
        (
            self.src, self.pair, self.half, self.inbox, self.zbuf, self.fin,
            self.pair_s, self.pair_r, self.rs_s, self.rs_r, self.z_s, self.z_r,
            self.ag_s, self.ag_r, self.back_s, self.back_r,
        ) = refs

    def swap_halves(self, pack_ref):
        for p in range(PIECES):
            self.src[p] = pack_ref[p * self.piece : (p + 1) * self.piece]
        place = self.place
        other = self.src.at[pl.ds((1 - place.c) * 16, 16)]
        self.pending = [place.remote(other, self.pair, self.pair_s.at[0], self.pair_r.at[0], place.sibling)]

    def arrived(self):
        for cp in self.pending:
            cp.wait_recv()

    def in_plane(self):
        place = self.place
        self.arrived()
        self.half[...] = self.src[pl.ds(place.c * 16, 16)] + self.pair[...]
        self.pending = []
        for d in PLANE_ORDER:
            index, peer = place.plane_peer(d)
            self.pending.append(
                place.remote(self.half.at[index], self.inbox.at[d], self.rs_s.at[d], self.rs_r.at[d], peer)
            )

    def along_z(self):
        self.arrived()
        own = self.half[self.place.plane]
        for d in range(1, 16):
            own = own + self.inbox[d]
        z = self.place.z
        self.zbuf[z] = own
        piece = self.zbuf.at[z]
        self.pending = [
            self.place.remote(piece, piece, self.z_s.at[d], self.z_r.at[d], self.place.z_peer(d)) for d in Z_ORDER
        ]

    def spread(self):
        place = self.place
        self.arrived()
        own = self.zbuf[0]
        for d in range(1, 8):
            own = own + self.zbuf[d]
        mine = place.c * 16 + place.plane
        self.fin[mine] = own
        piece = self.fin.at[mine]
        self.pending = [
            place.remote(piece, piece, self.ag_s.at[d], self.ag_r.at[d], place.plane_peer(d)[1]) for d in PLANE_ORDER
        ]
        self.backs = [place.remote(piece, piece, self.back_s.at[0], self.back_r.at[0], place.sibling)]

    def swap_back(self):
        place = self.place
        for d, cp in reversed(list(zip(PLANE_ORDER, self.pending))):
            cp.wait_recv()
            source = (4 - d // 4) % 4 * 4 + (4 - d % 4) % 4
            piece = self.fin.at[place.c * 16 + place.plane_peer(source)[0]]
            self.backs.append(place.remote(piece, piece, self.back_s.at[d], self.back_r.at[d], place.sibling))
        self.pending = self.backs

    def finish(self, out_ref):
        self.arrived()
        for p in range(PIECES):
            out_ref[p * self.piece : (p + 1) * self.piece] = self.fin[p]


def send_ghosts(place, ghost_ref, gbuf, send, recv):
    return [place.remote(ghost_ref.at[f], gbuf.at[f], send.at[f], recv.at[f], place.ghost_to[f]) for f in range(FACES)]


def add_ghosts(total, copies, gbuf, rows_ref):
    for f in range(FACES):
        copies[f].wait_recv()
        got = gbuf[f]
        high = got.astype(BF)
        low = (got - high.astype(F32)).astype(BF)
        ids = jnp.broadcast_to(rows_ref[f], (NODES, SLOTS))
        hot = jnp.where(ids == lax.broadcasted_iota(jnp.int32, (NODES, SLOTS), 0), 1.0, 0.0).astype(BF)
        total = total + (mm(hot, high) + mm(hot, low))
    return total


def fused_kernel(scales, *refs):
    inputs, refs = refs[:INPUTS], refs[INPUTS:]
    edge_out_ref, edge_sum_ref, node_sum_ref, node_out_ref = refs[:4]
    held, refs = refs[4 : 4 + INPUTS], refs[4 + INPUTS :]
    in_sem = refs[0]
    (
        table_t, full_t, z1, z2, sl1, sl2, nrm, inv, slo, shi, to_rows, to_cols, g1b, agg, acc, aggb, small, cols,
        w2t, w3t, w2h, w3h, node_h1, local_ref, ghost_out_ref, pack_ref, node_pack_ref,
    ) = refs[1:28]
    edge_comm, node_comm, (gbuf, g_s, g_r) = refs[28:44], refs[44:60], refs[60:]
    loads = [pltpu.make_async_copy(a, b, in_sem.at[k]) for k, (a, b) in enumerate(zip(inputs, held))]
    for cp in loads:
        cp.start()
    place = Place()
    place.greet()
    edge_reduce = AllReduce(place, EDGE_PIECE, edge_comm)
    node_reduce = AllReduce(place, NODE_PIECE, node_comm)
    (
        node_ref, ghost_ref, ew1_ref, ewh_ref, send_ref, recv_ref, edge_ref, eb_ref, eg_ref, es_ref,
        nw1_ref, nwh_ref, nb_ref, ng_ref, ncot_ref, ecot_ref, rows_ref,
    ) = held
    edge_scale, node_scale = scales
    for cp in loads[:4]:
        cp.wait()
    ghosts = ghost_ref[0, 0, 0].reshape(FACES * SLOTS, D)
    full_t[...] = jnp.concatenate([transposed(node_ref[0, 0, 0]), transposed(ghosts)], 1)
    table_t[:, 0:FULL] = mm(halved(transposed(ew1_ref[D : 2 * D])), full_t[...]).astype(BF)
    table_t[:, FULL + NODES :] = halved(transposed(ew1_ref[0:D]))
    w2t[...] = halved(transposed(ewh_ref[0]))
    w3t[...] = transposed(ewh_ref[1])
    w2h[...] = halved(ewh_ref[0])
    w3h[...] = halved(ewh_ref[1])
    node_pack_ref[ROW_NSM:] = jnp.zeros((NODE_ROWS - ROW_NSM, D), F32)
    pack_ref[ROW_ESM:] = jnp.zeros((EDGE_ROWS - ROW_ESM, D), F32)
    for cp in loads[4:14]:
        cp.wait()
    columns = [eb_ref[k : k + 1] for k in range(3)] + [eg_ref[...].reshape(1, D), es_ref[...].reshape(1, D)]
    columns += [nb_ref[k : k + 1] for k in range(3)] + [ng_ref[...].reshape(1, D)]
    halves = (0, 1, 5, 6)
    for k, column in enumerate(columns):
        cols[k] = jnp.broadcast_to(column * 0.5 if k in halves else column, (D, D)).T
    table_t[:, FULL : FULL + NODES] = (
        mm(halved(transposed(ew1_ref[2 * D : 3 * D])), full_t[:, 0:NODES]) + wide(cols[0], NODES)
    ).astype(BF)

    def forward(i):
        at = pl.ds(i * CH, CH)
        s_row = send_ref[0, 0, :, at]
        r_row = recv_ref[0, 0, :, at]
        to = jnp.concatenate(one_hot_rows(r_row, RECV_TILES), 0)
        to_rows[i] = to
        rhs = jnp.concatenate(one_hot_rows(s_row, SEND_TILES) + [to, transposed(edge_ref[0, 0, 0, at])], 0)
        p1 = mm(table_t[...], rhs)
        a1, d1 = silu_parts(p1)
        b1 = a1.astype(BF)
        z1[i] = b1
        sl1[i] = d1
        p2 = mm(w2t[...], b1) + wide(cols[1], CH)
        a2, d2 = silu_parts(p2)
        b2 = a2.astype(BF)
        z2[i] = b2
        sl2[i] = d2
        q = mm(w3t[...], b2) + wide(cols[2], CH)
        n, iv = norm_parts(q)
        nrm[i] = n
        inv[i] = iv
        new = (n * wide(cols[3], CH) + wide(cols[4], CH)).astype(BF)
        slo[at], shi[at] = column_digits(s_row)
        to = jnp.concatenate(one_hot_columns(*column_digits(r_row), RECV_TILES), 1)
        to_cols[at] = to
        part = mm(new, to)

        if i == 0:
            agg[...] = part
        else:
            agg[...] += part

    for i in range(CHUNKS):
        forward(i)

    for cp in loads[14:]:
        cp.wait()
    node_in = jnp.concatenate([full_t[:, 0:NODES], agg[...].astype(BF)], 0)
    a1, d1 = silu_parts(mm(halved(transposed(nw1_ref[...])), node_in) + wide(cols[5], NODES))
    b1 = a1.astype(BF)
    a2, d2 = silu_parts(mm(halved(transposed(nwh_ref[0])), b1) + wide(cols[6], NODES))
    b2 = a2.astype(BF)
    n, iv = norm_parts(mm(transposed(nwh_ref[1]), b2) + wide(cols[7], NODES))
    u = transposed(ncot_ref[0, 0, 0]).astype(F32)
    g3 = norm_back(u, wide(cols[8], NODES), n, iv)
    h3 = g3.astype(BF)
    g2 = mm(halved(nwh_ref[1]), h3) * d2
    h2 = g2.astype(BF)
    g1 = mm(halved(nwh_ref[0]), h2) * d1
    h1 = g1.astype(BF)
    node_h1[...] = h1
    aggb[...] = mm(nw1_ref[D : 2 * D], h1).astype(BF)
    node_pack_ref[0 : 2 * D] = mm_nt(node_in, h1) * node_scale
    node_pack_ref[ROW_NWH : ROW_NWH + D] = mm_nt(b1, h2) * node_scale
    node_pack_ref[ROW_NWH + D : ROW_NWH + 2 * D] = mm_nt(b2, h3) * node_scale
    node_pack_ref[ROW_NSM : ROW_NSM + 4] = node_scale * jnp.concatenate(
        [lane_sum(fold(g1)), lane_sum(fold(g2)), lane_sum(fold(g3)), lane_sum(fold(u * n))], 0
    )

    def backward(i):
        at = pl.ds(i * CH, CH)
        first = i == 0

        def add(ref, where, value):
            if first:
                ref[where] = value
            else:
                ref[where] += value

        cot = transposed(ecot_ref[0, 0, 0, at]).astype(F32)
        u = cot + mm(aggb[...], to_rows[i])
        n = nrm[i]
        g3 = norm_back(u, wide(cols[3], CH), n, inv[i])
        h3 = g3.astype(BF)
        g2 = mm(w3h[...], h3) * sl2[i]
        h2 = g2.astype(BF)
        g1 = mm(w2h[...], h2) * sl1[i]
        h1 = g1.astype(BF)
        g1b[i] = h1
        if i == 0:
            place.meet()
            node_reduce.swap_halves(node_pack_ref)
        ones = jnp.ones((16, CH), BF)
        for k, (z, h) in enumerate(((z1[i], h2), (z2[i], h3))):
            grad = mm_nt(jnp.concatenate([z, ones], 0), h)
            add(pack_ref, pl.ds(ROW_EWH + k * D, D), grad[0:D])
            add(pack_ref, pl.ds(ROW_ESM + 1 + k, 1), grad[D : D + 1])
        hot = one_hot_columns(slo[at], shi[at], SEND_TILES)
        add(acc, slice(None), mm(h1, jnp.concatenate(hot + [to_cols[at], edge_ref[0, 0, 0, at]], 1)))
        for k, x in enumerate((u * n, u)):
            add(small, k, fold(x))

    for i in range(CHUNKS):
        backward(i)
        if i == 0:
            node_reduce.in_plane()

    sums = acc[:, 0:FULL].astype(BF)
    sums_r = acc[:, FULL : FULL + NODES].astype(BF)
    pack_ref[0:D] = acc[:, FULL + NODES :].T * edge_scale
    pack_ref[D : 2 * D] = mm_nt(full_t[...], sums) * edge_scale
    pack_ref[2 * D : 3 * D] = mm_nt(full_t[:, 0:NODES], sums_r) * edge_scale
    pack_ref[ROW_EWH : ROW_EWH + 2 * D] = pack_ref[ROW_EWH : ROW_EWH + 2 * D] * edge_scale
    pack_ref[ROW_ESM + 1 : ROW_ESM + 3] = pack_ref[ROW_ESM + 1 : ROW_ESM + 3] * edge_scale
    pack_ref[ROW_ESM : ROW_ESM + 1] = lane_sum(fold(acc[:, FULL : FULL + NODES])) * edge_scale
    pack_ref[ROW_ESM + 3 : ROW_ESM + 5] = edge_scale * jnp.concatenate([lane_sum(small[0]), lane_sum(small[1])], 0)
    edge_reduce.swap_halves(pack_ref)
    back = mm_tn(sums, transposed(ew1_ref[D : 2 * D]))
    ghost_out_ref[...] = back[NODES:].reshape(FACES, SLOTS, D)
    edge_reduce.in_plane()
    ghosts = send_ghosts(place, ghost_out_ref, gbuf, g_s, g_r)
    local_ref[...] = (
        ncot_ref[0, 0, 0].astype(F32)
        + mm_tn(node_h1[...], transposed(nw1_ref[0:D]))
        + back[0:NODES]
        + mm_tn(sums_r, transposed(ew1_ref[2 * D : 3 * D]))
    )
    for i in range(CHUNKS):
        at = pl.ds(i * CH, CH)
        edge_out_ref[0, 0, 0, at] = (
            ecot_ref[0, 0, 0, at].astype(F32) + mm_tn(g1b[i], transposed(ew1_ref[0:D]))
        ).astype(BF)
    node_reduce.along_z()
    edge_reduce.along_z()
    node_out_ref[...] = add_ghosts(local_ref[...], ghosts, gbuf, rows_ref)
    node_reduce.spread()
    sent = len(place.started)
    edge_reduce.spread()
    node_reduce.swap_back()
    place.drain(sent)
    edge_reduce.swap_back()
    node_reduce.finish(node_sum_ref)
    place.drain(len(place.started))
    edge_reduce.finish(edge_sum_ref)


VMEM = pl.BlockSpec(memory_space=pltpu.VMEM)
HBM = pl.BlockSpec(memory_space=pltpu.HBM)
INPUTS = 17


def fused(args, scales):
    scratch = [pltpu.VMEM(a.shape, a.dtype) for a in args]
    scratch += [
        pltpu.SemaphoreType.DMA((INPUTS,)),
        pltpu.VMEM((D, FULL + NODES + D), BF),
        pltpu.VMEM((D, FULL), BF),
        pltpu.VMEM((CHUNKS, D, CH), BF),
        pltpu.VMEM((CHUNKS, D, CH), BF),
        pltpu.VMEM((CHUNKS, D, CH), F32),
        pltpu.VMEM((CHUNKS, D, CH), F32),
        pltpu.VMEM((CHUNKS, D, CH), F32),
        pltpu.VMEM((CHUNKS, 1, CH), F32),
        pltpu.VMEM((EDGES, D), BF),
        pltpu.VMEM((EDGES, D), BF),
        pltpu.VMEM((CHUNKS, NODES, CH), BF),
        pltpu.VMEM((EDGES, NODES), BF),
        pltpu.VMEM((CHUNKS, D, CH), BF),
        pltpu.VMEM((D, NODES), F32),
        pltpu.VMEM((D, FULL + NODES + D), F32),
        pltpu.VMEM((D, NODES), BF),
        pltpu.VMEM((2, D, D), F32),
        pltpu.VMEM((9, D, D), F32),
        pltpu.VMEM((D, D), BF),
        pltpu.VMEM((D, D), BF),
        pltpu.VMEM((D, D), BF),
        pltpu.VMEM((D, D), BF),
        pltpu.VMEM((D, NODES), BF),
        pltpu.VMEM((NODES, D), F32),
        pltpu.VMEM((FACES, SLOTS, D), F32),
        pltpu.VMEM((EDGE_ROWS, D), F32),
        pltpu.VMEM((NODE_ROWS, D), F32),
    ]
    for piece in (EDGE_PIECE, NODE_PIECE):
        scratch += [pltpu.VMEM((n, piece, D), F32) for n in (PIECES, 16, 16, 16, 8, PIECES)]
        scratch += [pltpu.SemaphoreType.DMA((n,)) for n in (1, 1, 16, 16, 8, 8, 16, 16, 16, 16)]
    scratch += [
        pltpu.VMEM((FACES, SLOTS, D), F32),
        pltpu.SemaphoreType.DMA((FACES,)),
        pltpu.SemaphoreType.DMA((FACES,)),
    ]
    return pl.pallas_call(
        functools.partial(fused_kernel, scales),
        out_shape=(
            jax.ShapeDtypeStruct((1, 1, 1, EDGES, D), BF),
            jax.ShapeDtypeStruct((EDGE_ROWS, D), F32),
            jax.ShapeDtypeStruct((NODE_ROWS, D), F32),
            jax.ShapeDtypeStruct((NODES, D), F32),
        ),
        in_specs=[HBM] * INPUTS,
        out_specs=(VMEM,) * 4,
        scratch_shapes=scratch,
        compiler_params=pltpu.CompilerParams(collective_id=0, has_side_effects=True, vmem_limit_bytes=52 * 2**20),
        cost_estimate=pl.CostEstimate(flops=6_000_000_000, bytes_accessed=6_000_000, transcendentals=800_000),
    )(*[pltpu.with_memory_space_constraint(a, pltpu.HBM) for a in args])


def unpack_kernel(
    edge_in, edge_sum, node_sum, node_in,
    edge_out, node_out, ew1, ewh, nw1, nwh, eb, eg, es, nb, ng,
    eb_v, eg_v, es_v, nb_v, ng_v, sem,
):
    eb_v[...] = edge_sum[ROW_ESM : ROW_ESM + 3]
    eg_v[...] = edge_sum[ROW_ESM + 3 : ROW_ESM + 4].reshape(D)
    es_v[...] = edge_sum[ROW_ESM + 4 : ROW_ESM + 5].reshape(D)
    nb_v[...] = node_sum[ROW_NSM : ROW_NSM + 3]
    ng_v[...] = node_sum[ROW_NSM + 3 : ROW_NSM + 4].reshape(D)
    moves = (
        (edge_in, edge_out),
        (node_in, node_out.at[0, 0, 0]),
        (edge_sum.at[0 : 3 * D], ew1),
        (edge_sum.at[ROW_EWH : ROW_EWH + D], ewh.at[0]),
        (edge_sum.at[ROW_EWH + D : ROW_EWH + 2 * D], ewh.at[1]),
        (node_sum.at[0 : 2 * D], nw1),
        (node_sum.at[ROW_NWH : ROW_NWH + D], nwh.at[0]),
        (node_sum.at[ROW_NWH + D : ROW_NWH + 2 * D], nwh.at[1]),
        (eb_v, eb),
        (eg_v, eg),
        (es_v, es),
        (nb_v, nb),
        (ng_v, ng),
    )
    copies = [pltpu.make_async_copy(a, b, sem.at[k]) for k, (a, b) in enumerate(moves)]
    for cp in copies:
        cp.start()
    for cp in copies:
        cp.wait()


def unpack(edge, edge_sum, node_sum, node):
    shapes = ((1, 1, 1, NODES, D), (3 * D, D), (2, D, D), (2 * D, D), (2, D, D), (3, D), (D,), (D,), (3, D), (D,))
    return pl.pallas_call(
        unpack_kernel,
        out_shape=(jax.ShapeDtypeStruct(edge.shape, BF),) + tuple(jax.ShapeDtypeStruct(s, F32) for s in shapes),
        in_specs=[VMEM] * 4,
        out_specs=(HBM,) * 11,
        scratch_shapes=[pltpu.VMEM(s, F32) for s in shapes[5:]] + [pltpu.SemaphoreType.DMA((13,))],
        compiler_params=pltpu.CompilerParams(vmem_limit_bytes=8 * 2**20),
        cost_estimate=pl.CostEstimate(flops=1_000_000, bytes_accessed=4_000_000, transcendentals=0),
    )(edge, edge_sum, node_sum, node)


def on_device(
    node_latent, ghost_latent, edge_latent, senders, receivers, export_rows, node_cotangent, edge_cotangent,
    w_edge_in, w_edge_hidden, b_edge, gain_edge, shift_edge, w_node_in, w_node_hidden, b_node, gain_node,
):
    devices = lax.axis_size("gx") * lax.axis_size("gy") * lax.axis_size("gz")
    scales = (float(EDGES * devices) ** (-0.5), float(NODES * devices) ** (-0.5))
    edge, edge_sum, node_sum, node = fused(
        (
            node_latent, ghost_latent, w_edge_in, w_edge_hidden, senders, receivers, edge_latent,
            b_edge, gain_edge, shift_edge, w_node_in, w_node_hidden, b_node, gain_node,
            node_cotangent, edge_cotangent, export_rows.reshape(FACES, 1, SLOTS),
        ),
        scales,
    )
    edge_grad, node_grad, ew1, ewh, nw1, nwh, eb, eg, es, nb, ng = unpack(edge, edge_sum, node_sum, node)
    return (node_grad, edge_grad, ew1, ewh, eb, eg, es, nw1, nwh, nb, ng)


def solution(mesh):
    block = lambda dims: P("gx", "gy", "gz", *([None] * dims))
    in_specs = tuple(block(k) for k in (2, 3, 2, 1, 1, 2, 2, 2)) + (P(),) * 9
    out_specs = (block(2), block(2)) + (P(),) * 9
    return jax.shard_map(on_device, mesh=mesh, in_specs=in_specs, out_specs=out_specs, check_vma=False)
```

```python
import functools

import jax
import jax.numpy as jnp
from jax import lax
from jax.experimental import pallas as pl
from jax.experimental.pallas import tpu as pltpu
from jax.sharding import PartitionSpec as P

EPSILON = 1e-05
MESH = pl.DeviceIdType.MESH
BF = jnp.bfloat16
F32 = jnp.float32
D = 128
NODES = 512
FACES = 6
SLOTS = 64
FULL = NODES + FACES * SLOTS
EDGES = 2816
CH = 2816
CHUNKS = EDGES // CH
SEND_TILES = FULL // D
RECV_TILES = NODES // D
TILES = SEND_TILES + RECV_TILES
PIECES = 32
EDGE_PIECE = 21
NODE_PIECE = 17
EDGE_ROWS = PIECES * EDGE_PIECE
NODE_ROWS = PIECES * NODE_PIECE
ROW_EWH = 3 * D
ROW_ESM = 5 * D
ROW_NWH = 2 * D
ROW_NSM = 4 * D


PLANE_ORDER = (10, 9, 11, 6, 14, 2, 8, 5, 7, 13, 15, 1, 3, 4, 12)
Z_ORDER = (4, 3, 5, 2, 6, 1, 7)


def mm(a, b):
    return jnp.dot(a, b, preferred_element_type=F32)


def mm_tn(a, b):
    return lax.dot_general(a, b, (((0,), (0,)), ((), ())), preferred_element_type=F32)


def mm_nt(a, b):
    return lax.dot_general(a, b, (((1,), (1,)), ((), ())), preferred_element_type=F32)


def transposed(w):
    return w.T


def halved(w):
    return (w.astype(F32) * 0.5).astype(BF)


def silu_parts(h):
    t = jnp.tanh(h)
    z = h + h * t
    return z, (1.0 + t) + z * (1.0 - t)


def norm_parts(p):
    c = p - jnp.mean(p, 0, keepdims=True)
    inv = lax.rsqrt(jnp.mean(c * c, 0, keepdims=True) + EPSILON)
    return c * inv, inv


def norm_back(u, gain, n, inv):
    t = u * gain
    return inv * (t - jnp.mean(t, 0, keepdims=True) - n * jnp.mean(t * n, 0, keepdims=True))


def wide(column, n):
    return jnp.concatenate([column] * (n // D), 1)


def fold(x):
    total = x[:, 0:D]
    for k in range(1, x.shape[1] // D):
        total = total + x[:, k * D : (k + 1) * D]
    return total


def lane_sum(x):
    return jnp.sum(x.T, 0, keepdims=True)


def column_digits(ids_row):
    parts = []
    for digit in (ids_row & (D - 1), ids_row >> 7):
        row = digit.astype(F32)
        tiles = [
            jnp.broadcast_to(row[:, j : j + D], (D, D)).astype(BF).T for j in range(0, ids_row.shape[1], D)
        ]
        parts.append(jnp.concatenate(tiles, 0))
    return parts


def one_hot_columns(lo, hi, tiles):
    lane = lax.broadcasted_iota(jnp.int32, lo.shape, 1).astype(F32).astype(BF)
    zero = jnp.zeros(lo.shape, BF)
    base = jnp.where(lo == lane, jnp.ones(lo.shape, BF), zero)
    return [jnp.where(hi == BF(k), base, zero) for k in range(tiles)]


def one_hot_rows(ids_row, tiles):
    n = ids_row.shape[1]
    lo = jnp.broadcast_to((ids_row & (D - 1)).astype(F32), (D, n)).astype(BF)
    hi = jnp.broadcast_to((ids_row >> 7).astype(F32), (D, n)).astype(BF)
    row = lax.broadcasted_iota(jnp.int32, (D, n), 0).astype(F32).astype(BF)
    zero = jnp.zeros((D, n), BF)
    base = jnp.where(lo == row, jnp.ones((D, n), BF), zero)
    return [jnp.where(hi == BF(k), base, zero) for k in range(tiles)]


class Bytes:
    def __init__(self, ref, sem):
        self.copy = pltpu.make_async_copy(ref, ref, sem)

    def wait_recv(self):
        self.copy.wait()

    def wait_send(self):
        self.copy.wait()


class Place:
    def __init__(self):
        gx, gy, gz = lax.axis_index("gx"), lax.axis_index("gy"), lax.axis_index("gz")
        self.y, self.zl = gx // 2, gx % 2
        self.x, self.c = gz // 2, gz % 2
        self.z = gy * 2 + self.zl
        self.at = (gx, gy, gz)
        self.plane = self.x * 4 + self.y
        self.sibling = (gx, gy, gz + 1 - 2 * self.c)
        self.started = []
        self.ghost_to = []
        for f in range(FACES):
            step = 1 if f % 2 == 0 else -1
            self.ghost_to.append((
                ((gx + step + 8) % 8, gy, gz),
                (gx, (gy + step + 4) % 4, gz),
                (gx, gy, (gz + step + 8) % 8),
            )[f // 2])

    def plane_peer(self, d):
        px, py = (self.x + d // 4) % 4, (self.y + d % 4) % 4
        return px * 4 + py, (py * 2 + self.zl, self.at[1], px * 2 + self.c)

    def z_peer(self, d):
        pz = (self.z + d) % 8
        return (self.y * 2 + pz % 2, pz // 2, self.at[2])

    def greet(self):
        barrier = pltpu.get_barrier_semaphore()
        peers = [self.sibling] + [self.plane_peer(d)[1] for d in PLANE_ORDER]
        peers += [self.z_peer(d) for d in Z_ORDER] + self.ghost_to
        for peer in peers:
            pl.semaphore_signal(barrier, inc=1, device_id=peer, device_id_type=MESH)
        self.greeted = len(peers)

    def meet(self):
        pl.semaphore_wait(pltpu.get_barrier_semaphore(), self.greeted)

    def remote(self, src, dst, send, recv, peer, keep=True):
        cp = pltpu.make_async_remote_copy(
            src_ref=src, dst_ref=dst, send_sem=send, recv_sem=recv, device_id=peer, device_id_type=MESH
        )
        cp.start()
        if keep:
            self.started.append(cp)
        return cp

    def sent(self, ref, sem):
        self.started.append(Bytes(ref, sem))

    def drain(self, count):
        for cp in self.started[:count]:
            cp.wait_send()
        self.started = self.started[count:]


class AllReduce:
    def __init__(self, place, piece, refs):
        self.place, self.piece = place, piece
        (
            self.src, self.pair, self.half, self.inbox, self.zbuf, self.fin,
            self.pair_s, self.pair_r, self.rs_s, self.rs_r, self.z_s, self.z_r,
            self.ag_s, self.ag_r, self.back_s, self.back_r,
        ) = refs

    def swap_halves(self, pack_ref):
        for p in range(PIECES):
            self.src[p] = pack_ref[p * self.piece : (p + 1) * self.piece]
        place = self.place
        other = self.src.at[pl.ds((1 - place.c) * 16, 16)]
        self.pending = [place.remote(other, self.pair, self.pair_s.at[0], self.pair_r.at[0], place.sibling)]

    def arrived(self):
        for cp in self.pending:
            cp.wait_recv()

    def in_plane(self):
        place = self.place
        self.arrived()
        self.half[...] = self.src[pl.ds(place.c * 16, 16)] + self.pair[...]
        for d in PLANE_ORDER:
            index, peer = place.plane_peer(d)
            place.remote(self.half.at[index], self.inbox.at[d], self.rs_s.at[0], self.rs_r.at[0], peer, keep=False)
        place.sent(self.half.at[0:15], self.rs_s.at[0])
        self.pending = [Bytes(self.inbox.at[1:16], self.rs_r.at[0])]

    def along_z(self):
        self.arrived()
        own = self.half[self.place.plane]
        for d in range(1, 16):
            own = own + self.inbox[d]
        z = self.place.z
        self.zbuf[z] = own
        piece = self.zbuf.at[z]
        for d in Z_ORDER:
            self.place.remote(piece, piece, self.z_s.at[0], self.z_r.at[0], self.place.z_peer(d), keep=False)
        self.place.sent(self.zbuf.at[0:7], self.z_s.at[0])
        self.pending = [Bytes(self.zbuf.at[0:7], self.z_r.at[0])]

    def spread(self):
        place = self.place
        self.arrived()
        own = self.zbuf[0]
        for d in range(1, 8):
            own = own + self.zbuf[d]
        mine = place.c * 16 + place.plane
        self.fin[mine] = own
        piece = self.fin.at[mine]
        self.pending = [
            place.remote(piece, piece, self.ag_s.at[0], self.ag_r.at[d], place.plane_peer(d)[1], keep=False)
            for d in PLANE_ORDER
        ]
        place.sent(self.fin.at[0:15], self.ag_s.at[0])
        place.remote(piece, piece, self.back_s.at[0], self.back_r.at[0], place.sibling, keep=False)

    def swap_back(self):
        place = self.place
        for d, cp in reversed(list(zip(PLANE_ORDER, self.pending))):
            cp.wait_recv()
            source = (4 - d // 4) % 4 * 4 + (4 - d % 4) % 4
            piece = self.fin.at[place.c * 16 + place.plane_peer(source)[0]]
            place.remote(piece, piece, self.back_s.at[0], self.back_r.at[0], place.sibling, keep=False)
        place.sent(self.fin.at[0:16], self.back_s.at[0])
        self.pending = [Bytes(self.fin.at[0:16], self.back_r.at[0])]

    def finish(self, out_ref):
        self.arrived()
        for p in range(PIECES):
            out_ref[p * self.piece : (p + 1) * self.piece] = self.fin[p]


def send_ghosts(place, ghost_ref, gbuf, send, recv):
    return [place.remote(ghost_ref.at[f], gbuf.at[f], send.at[f], recv.at[f], place.ghost_to[f]) for f in range(FACES)]


def add_ghosts(total, copies, gbuf, rows_ref):
    for f in range(FACES):
        copies[f].wait_recv()
        got = gbuf[f]
        high = got.astype(BF)
        low = (got - high.astype(F32)).astype(BF)
        ids = jnp.broadcast_to(rows_ref[f], (NODES, SLOTS))
        hot = jnp.where(ids == lax.broadcasted_iota(jnp.int32, (NODES, SLOTS), 0), 1.0, 0.0).astype(BF)
        total = total + (mm(hot, high) + mm(hot, low))
    return total


def fused_kernel(scales, *refs):
    inputs, refs = refs[:INPUTS], refs[INPUTS:]
    edge_out_ref, edge_sum_ref, node_sum_ref, node_out_ref = refs[:4]
    held, refs = refs[4 : 4 + INPUTS], refs[4 + INPUTS :]
    in_sem = refs[0]
    (
        table_t, full_t, z1, z2, sl1, sl2, nrm, inv, slo, shi, to_rows, to_cols, g1b, agg, acc, aggb, small, cols,
        w2t, w3t, w2h, w3h, node_h1, local_ref, ghost_out_ref, pack_ref, node_pack_ref,
    ) = refs[1:28]
    edge_comm, node_comm, (gbuf, g_s, g_r) = refs[28:44], refs[44:60], refs[60:]
    loads = [pltpu.make_async_copy(a, b, in_sem.at[k]) for k, (a, b) in enumerate(zip(inputs, held))]
    for cp in loads:
        cp.start()
    place = Place()
    place.greet()
    edge_reduce = AllReduce(place, EDGE_PIECE, edge_comm)
    node_reduce = AllReduce(place, NODE_PIECE, node_comm)
    (
        node_ref, ghost_ref, ew1_ref, ewh_ref, send_ref, recv_ref, edge_ref, eb_ref, eg_ref, es_ref,
        nw1_ref, nwh_ref, nb_ref, ng_ref, ncot_ref, ecot_ref, rows_ref,
    ) = held
    edge_scale, node_scale = scales
    for cp in loads[:4]:
        cp.wait()
    ghosts = ghost_ref[0, 0, 0].reshape(FACES * SLOTS, D)
    full_t[...] = jnp.concatenate([transposed(node_ref[0, 0, 0]), transposed(ghosts)], 1)
    table_t[:, 0:FULL] = mm(halved(transposed(ew1_ref[D : 2 * D])), full_t[...]).astype(BF)
    table_t[:, FULL + NODES :] = halved(transposed(ew1_ref[0:D]))
    w2t[...] = halved(transposed(ewh_ref[0]))
    w3t[...] = transposed(ewh_ref[1])
    w2h[...] = halved(ewh_ref[0])
    w3h[...] = halved(ewh_ref[1])
    node_pack_ref[ROW_NSM:] = jnp.zeros((NODE_ROWS - ROW_NSM, D), F32)
    pack_ref[ROW_ESM:] = jnp.zeros((EDGE_ROWS - ROW_ESM, D), F32)
    for cp in loads[4:14]:
        cp.wait()
    columns = [eb_ref[k : k + 1] for k in range(3)] + [eg_ref[...].reshape(1, D), es_ref[...].reshape(1, D)]
    columns += [nb_ref[k : k + 1] for k in range(3)] + [ng_ref[...].reshape(1, D)]
    halves = (0, 1, 5, 6)
    for k, column in enumerate(columns):
        cols[k] = jnp.broadcast_to(column * 0.5 if k in halves else column, (D, D)).T
    table_t[:, FULL : FULL + NODES] = (
        mm(halved(transposed(ew1_ref[2 * D : 3 * D])), full_t[:, 0:NODES]) + wide(cols[0], NODES)
    ).astype(BF)

    def forward(i):
        at = pl.ds(i * CH, CH)
        s_row = send_ref[0, 0, :, at]
        r_row = recv_ref[0, 0, :, at]
        to = jnp.concatenate(one_hot_rows(r_row, RECV_TILES), 0)
        to_rows[i] = to
        rhs = jnp.concatenate(one_hot_rows(s_row, SEND_TILES) + [to, transposed(edge_ref[0, 0, 0, at])], 0)
        p1 = mm(table_t[...], rhs)
        a1, d1 = silu_parts(p1)
        b1 = a1.astype(BF)
        z1[i] = b1
        sl1[i] = d1
        p2 = mm(w2t[...], b1) + wide(cols[1], CH)
        a2, d2 = silu_parts(p2)
        b2 = a2.astype(BF)
        z2[i] = b2
        sl2[i] = d2
        q = mm(w3t[...], b2) + wide(cols[2], CH)
        n, iv = norm_parts(q)
        nrm[i] = n
        inv[i] = iv
        new = (n * wide(cols[3], CH) + wide(cols[4], CH)).astype(BF)
        slo[at], shi[at] = column_digits(s_row)
        to = jnp.concatenate(one_hot_columns(*column_digits(r_row), RECV_TILES), 1)
        to_cols[at] = to
        part = mm(new, to)

        if i == 0:
            agg[...] = part
        else:
            agg[...] += part

    for i in range(CHUNKS):
        forward(i)

    for cp in loads[14:]:
        cp.wait()
    node_in = jnp.concatenate([full_t[:, 0:NODES], agg[...].astype(BF)], 0)
    a1, d1 = silu_parts(mm(halved(transposed(nw1_ref[...])), node_in) + wide(cols[5], NODES))
    b1 = a1.astype(BF)
    a2, d2 = silu_parts(mm(halved(transposed(nwh_ref[0])), b1) + wide(cols[6], NODES))
    b2 = a2.astype(BF)
    n, iv = norm_parts(mm(transposed(nwh_ref[1]), b2) + wide(cols[7], NODES))
    u = transposed(ncot_ref[0, 0, 0]).astype(F32)
    g3 = norm_back(u, wide(cols[8], NODES), n, iv)
    h3 = g3.astype(BF)
    g2 = mm(halved(nwh_ref[1]), h3) * d2
    h2 = g2.astype(BF)
    g1 = mm(halved(nwh_ref[0]), h2) * d1
    h1 = g1.astype(BF)
    node_h1[...] = h1
    aggb[...] = mm(nw1_ref[D : 2 * D], h1).astype(BF)
    node_pack_ref[0 : 2 * D] = mm_nt(node_in, h1) * node_scale
    node_pack_ref[ROW_NWH : ROW_NWH + D] = mm_nt(b1, h2) * node_scale
    node_pack_ref[ROW_NWH + D : ROW_NWH + 2 * D] = mm_nt(b2, h3) * node_scale
    node_pack_ref[ROW_NSM : ROW_NSM + 4] = node_scale * jnp.concatenate(
        [lane_sum(fold(g1)), lane_sum(fold(g2)), lane_sum(fold(g3)), lane_sum(fold(u * n))], 0
    )

    def backward(i):
        at = pl.ds(i * CH, CH)
        first = i == 0

        def add(ref, where, value):
            if first:
                ref[where] = value
            else:
                ref[where] += value

        cot = transposed(ecot_ref[0, 0, 0, at]).astype(F32)
        u = cot + mm(aggb[...], to_rows[i])
        n = nrm[i]
        g3 = norm_back(u, wide(cols[3], CH), n, inv[i])
        h3 = g3.astype(BF)
        g2 = mm(w3h[...], h3) * sl2[i]
        h2 = g2.astype(BF)
        g1 = mm(w2h[...], h2) * sl1[i]
        h1 = g1.astype(BF)
        g1b[i] = h1
        if i == 0:
            place.meet()
            node_reduce.swap_halves(node_pack_ref)
        ones = jnp.ones((16, CH), BF)
        for k, (z, h) in enumerate(((z1[i], h2), (z2[i], h3))):
            grad = mm_nt(jnp.concatenate([z, ones], 0), h)
            add(pack_ref, pl.ds(ROW_EWH + k * D, D), grad[0:D])
            add(pack_ref, pl.ds(ROW_ESM + 1 + k, 1), grad[D : D + 1])
        hot = one_hot_columns(slo[at], shi[at], SEND_TILES)
        add(acc, slice(None), mm(h1, jnp.concatenate(hot + [to_cols[at], edge_ref[0, 0, 0, at]], 1)))
        for k, x in enumerate((u * n, u)):
            add(small, k, fold(x))

    for i in range(CHUNKS):
        backward(i)
        if i == 0:
            node_reduce.in_plane()

    sums = acc[:, 0:FULL].astype(BF)
    sums_r = acc[:, FULL : FULL + NODES].astype(BF)
    pack_ref[0:D] = acc[:, FULL + NODES :].T * edge_scale
    pack_ref[D : 2 * D] = mm_nt(full_t[...], sums) * edge_scale
    pack_ref[2 * D : 3 * D] = mm_nt(full_t[:, 0:NODES], sums_r) * edge_scale
    pack_ref[ROW_EWH : ROW_EWH + 2 * D] = pack_ref[ROW_EWH : ROW_EWH + 2 * D] * edge_scale
    pack_ref[ROW_ESM + 1 : ROW_ESM + 3] = pack_ref[ROW_ESM + 1 : ROW_ESM + 3] * edge_scale
    pack_ref[ROW_ESM : ROW_ESM + 1] = lane_sum(fold(acc[:, FULL : FULL + NODES])) * edge_scale
    pack_ref[ROW_ESM + 3 : ROW_ESM + 5] = edge_scale * jnp.concatenate([lane_sum(small[0]), lane_sum(small[1])], 0)
    edge_reduce.swap_halves(pack_ref)
    back = mm_tn(sums, transposed(ew1_ref[D : 2 * D]))
    ghost_out_ref[...] = back[NODES:].reshape(FACES, SLOTS, D)
    edge_reduce.in_plane()
    ghosts = send_ghosts(place, ghost_out_ref, gbuf, g_s, g_r)
    local_ref[...] = (
        ncot_ref[0, 0, 0].astype(F32)
        + mm_tn(node_h1[...], transposed(nw1_ref[0:D]))
        + back[0:NODES]
        + mm_tn(sums_r, transposed(ew1_ref[2 * D : 3 * D]))
    )
    for i in range(CHUNKS):
        at = pl.ds(i * CH, CH)
        edge_out_ref[0, 0, 0, at] = (
            ecot_ref[0, 0, 0, at].astype(F32) + mm_tn(g1b[i], transposed(ew1_ref[0:D]))
        ).astype(BF)
    node_reduce.along_z()
    edge_reduce.along_z()
    node_out_ref[...] = add_ghosts(local_ref[...], ghosts, gbuf, rows_ref)
    node_reduce.spread()
    sent = len(place.started)
    edge_reduce.spread()
    node_reduce.swap_back()
    place.drain(sent)
    edge_reduce.swap_back()
    node_reduce.finish(node_sum_ref)
    place.drain(len(place.started))
    edge_reduce.finish(edge_sum_ref)


VMEM = pl.BlockSpec(memory_space=pltpu.VMEM)
HBM = pl.BlockSpec(memory_space=pltpu.HBM)
INPUTS = 17


def fused(args, scales):
    scratch = [pltpu.VMEM(a.shape, a.dtype) for a in args]
    scratch += [
        pltpu.SemaphoreType.DMA((INPUTS,)),
        pltpu.VMEM((D, FULL + NODES + D), BF),
        pltpu.VMEM((D, FULL), BF),
        pltpu.VMEM((CHUNKS, D, CH), BF),
        pltpu.VMEM((CHUNKS, D, CH), BF),
        pltpu.VMEM((CHUNKS, D, CH), F32),
        pltpu.VMEM((CHUNKS, D, CH), F32),
        pltpu.VMEM((CHUNKS, D, CH), F32),
        pltpu.VMEM((CHUNKS, 1, CH), F32),
        pltpu.VMEM((EDGES, D), BF),
        pltpu.VMEM((EDGES, D), BF),
        pltpu.VMEM((CHUNKS, NODES, CH), BF),
        pltpu.VMEM((EDGES, NODES), BF),
        pltpu.VMEM((CHUNKS, D, CH), BF),
        pltpu.VMEM((D, NODES), F32),
        pltpu.VMEM((D, FULL + NODES + D), F32),
        pltpu.VMEM((D, NODES), BF),
        pltpu.VMEM((2, D, D), F32),
        pltpu.VMEM((9, D, D), F32),
        pltpu.VMEM((D, D), BF),
        pltpu.VMEM((D, D), BF),
        pltpu.VMEM((D, D), BF),
        pltpu.VMEM((D, D), BF),
        pltpu.VMEM((D, NODES), BF),
        pltpu.VMEM((NODES, D), F32),
        pltpu.VMEM((FACES, SLOTS, D), F32),
        pltpu.VMEM((EDGE_ROWS, D), F32),
        pltpu.VMEM((NODE_ROWS, D), F32),
    ]
    for piece in (EDGE_PIECE, NODE_PIECE):
        scratch += [pltpu.VMEM((n, piece, D), F32) for n in (PIECES, 16, 16, 16, 8, PIECES)]
        scratch += [pltpu.SemaphoreType.DMA((n,)) for n in (1, 1, 1, 1, 1, 1, 1, 16, 1, 1)]
    scratch += [
        pltpu.VMEM((FACES, SLOTS, D), F32),
        pltpu.SemaphoreType.DMA((FACES,)),
        pltpu.SemaphoreType.DMA((FACES,)),
    ]
    return pl.pallas_call(
        functools.partial(fused_kernel, scales),
        out_shape=(
            jax.ShapeDtypeStruct((1, 1, 1, EDGES, D), BF),
            jax.ShapeDtypeStruct((EDGE_ROWS, D), F32),
            jax.ShapeDtypeStruct((NODE_ROWS, D), F32),
            jax.ShapeDtypeStruct((NODES, D), F32),
        ),
        in_specs=[HBM] * INPUTS,
        out_specs=(VMEM,) * 4,
        scratch_shapes=scratch,
        compiler_params=pltpu.CompilerParams(collective_id=0, has_side_effects=True, vmem_limit_bytes=52 * 2**20),
        cost_estimate=pl.CostEstimate(flops=6_000_000_000, bytes_accessed=6_000_000, transcendentals=800_000),
    )(*[pltpu.with_memory_space_constraint(a, pltpu.HBM) for a in args])


def unpack_kernel(
    edge_in, edge_sum, node_sum, node_in,
    edge_out, node_out, ew1, ewh, nw1, nwh, eb, eg, es, nb, ng,
    eb_v, eg_v, es_v, nb_v, ng_v, sem,
):
    eb_v[...] = edge_sum[ROW_ESM : ROW_ESM + 3]
    eg_v[...] = edge_sum[ROW_ESM + 3 : ROW_ESM + 4].reshape(D)
    es_v[...] = edge_sum[ROW_ESM + 4 : ROW_ESM + 5].reshape(D)
    nb_v[...] = node_sum[ROW_NSM : ROW_NSM + 3]
    ng_v[...] = node_sum[ROW_NSM + 3 : ROW_NSM + 4].reshape(D)
    moves = (
        (edge_in, edge_out),
        (node_in, node_out.at[0, 0, 0]),
        (edge_sum.at[0 : 3 * D], ew1),
        (edge_sum.at[ROW_EWH : ROW_EWH + D], ewh.at[0]),
        (edge_sum.at[ROW_EWH + D : ROW_EWH + 2 * D], ewh.at[1]),
        (node_sum.at[0 : 2 * D], nw1),
        (node_sum.at[ROW_NWH : ROW_NWH + D], nwh.at[0]),
        (node_sum.at[ROW_NWH + D : ROW_NWH + 2 * D], nwh.at[1]),
        (eb_v, eb),
        (eg_v, eg),
        (es_v, es),
        (nb_v, nb),
        (ng_v, ng),
    )
    copies = [pltpu.make_async_copy(a, b, sem.at[k]) for k, (a, b) in enumerate(moves)]
    for cp in copies:
        cp.start()
    for cp in copies:
        cp.wait()


def unpack(edge, edge_sum, node_sum, node):
    shapes = ((1, 1, 1, NODES, D), (3 * D, D), (2, D, D), (2 * D, D), (2, D, D), (3, D), (D,), (D,), (3, D), (D,))
    return pl.pallas_call(
        unpack_kernel,
        out_shape=(jax.ShapeDtypeStruct(edge.shape, BF),) + tuple(jax.ShapeDtypeStruct(s, F32) for s in shapes),
        in_specs=[VMEM] * 4,
        out_specs=(HBM,) * 11,
        scratch_shapes=[pltpu.VMEM(s, F32) for s in shapes[5:]] + [pltpu.SemaphoreType.DMA((13,))],
        compiler_params=pltpu.CompilerParams(vmem_limit_bytes=8 * 2**20),
        cost_estimate=pl.CostEstimate(flops=1_000_000, bytes_accessed=4_000_000, transcendentals=0),
    )(edge, edge_sum, node_sum, node)


def on_device(
    node_latent, ghost_latent, edge_latent, senders, receivers, export_rows, node_cotangent, edge_cotangent,
    w_edge_in, w_edge_hidden, b_edge, gain_edge, shift_edge, w_node_in, w_node_hidden, b_node, gain_node,
):
    devices = lax.axis_size("gx") * lax.axis_size("gy") * lax.axis_size("gz")
    scales = (float(EDGES * devices) ** (-0.5), float(NODES * devices) ** (-0.5))
    edge, edge_sum, node_sum, node = fused(
        (
            node_latent, ghost_latent, w_edge_in, w_edge_hidden, senders, receivers, edge_latent,
            b_edge, gain_edge, shift_edge, w_node_in, w_node_hidden, b_node, gain_node,
            node_cotangent, edge_cotangent, export_rows.reshape(FACES, 1, SLOTS),
        ),
        scales,
    )
    edge_grad, node_grad, ew1, ewh, nw1, nwh, eb, eg, es, nb, ng = unpack(edge, edge_sum, node_sum, node)
    return (node_grad, edge_grad, ew1, ewh, eb, eg, es, nw1, nwh, nb, ng)


def solution(mesh):
    block = lambda dims: P("gx", "gy", "gz", *([None] * dims))
    in_specs = tuple(block(k) for k in (2, 3, 2, 1, 1, 2, 2, 2)) + (P(),) * 9
    out_specs = (block(2), block(2)) + (P(),) * 9
    return jax.shard_map(on_device, mesh=mesh, in_specs=in_specs, out_specs=out_specs, check_vma=False)
```
